8 devices in a mesh: problem: 1 (over z), samp: 2 (over y), feat: 4 (over x, core).
Axes of the slice: x: 2, y: 2, z: 1, core: 2. Of those that a mesh axis runs over, the one named last changes fastest.
Arguments:
- design: bfloat16 [4096, 131072], P(('problem', 'samp'), 'feat')
- targets: float32 [4096, 128], P(('problem', 'samp'))
- coef_init: float32 [131072, 128], P(('problem', 'feat'))
- step_sizes: float32 [131072], P(('problem', 'feat'))
- ridge_weights: float32 [128], P('problem')
Outputs:
- output 1: float32 [131072, 128], P(('problem', 'feat'))
- output 2: float32 [4096, 128], P(('problem', 'samp'))
All inputs are finite; a program needn't handle non-finite values.
Results may differ from the reference program's by a relative error of at most 0.00677784.
Values are sent between devices in bfloat16 or wider.
A program may use at most 1 GiB of HBM per device.

```python
import jax
import jax.numpy as jnp
from jax import lax

NUM_ROWS = 4096
NUM_FEATURES = 131072
NUM_TARGETS = 128
FEAT_BLOCKS = 4
SWEEPS = 4
STEP_WEIGHT = 0.5


def setup_inputs(seed: int = 0, part: int = 0) -> dict:
    base_key = jax.random.fold_in(jax.random.key(seed), part)
    sub_keys = jax.random.split(base_key, 9)
    shared_rank = 8
    shared_mix = 0.8
    row_block = NUM_ROWS // 8
    factors = jax.random.normal(sub_keys[0], (NUM_ROWS, shared_rank), jnp.float32)
    loadings = jax.random.normal(sub_keys[1], (shared_rank, NUM_FEATURES), jnp.float32)

    def draw_rows(block_index):
        rows_f = lax.dynamic_slice_in_dim(factors, block_index * row_block, row_block, 0)
        shared = jnp.dot(rows_f, loadings) * (shared_mix / shared_rank) ** 0.5
        noise_blk = jax.random.normal(jax.random.fold_in(sub_keys[2], block_index), (row_block, NUM_FEATURES), jnp.float32)
        return (shared + (1.0 - shared_mix) ** 0.5 * noise_blk).astype(jnp.bfloat16)

    design = lax.map(draw_rows, jnp.arange(8)).reshape(NUM_ROWS, NUM_FEATURES)

    def power_step(step_index, probe_vec):
        unit_vec = probe_vec / jnp.linalg.norm(probe_vec)
        image_vec = jnp.dot(design, unit_vec.astype(jnp.bfloat16), preferred_element_type=jnp.float32)
        return jnp.dot(image_vec.astype(jnp.bfloat16), design, preferred_element_type=jnp.float32) / NUM_ROWS

    probe_init = jax.random.normal(sub_keys[3], (NUM_FEATURES,), jnp.float32)
    curvature = 1.15 * jnp.linalg.norm(lax.fori_loop(0, 12, power_step, probe_init))
    step_sizes = jax.random.uniform(sub_keys[4], (NUM_FEATURES,), jnp.float32, 0.4, 0.8) / curvature
    ridge_weights = jax.random.uniform(sub_keys[5], (NUM_TARGETS,), jnp.float32, 0.05, 0.25) * curvature
    coef_init = jax.random.normal(sub_keys[6], (NUM_FEATURES, NUM_TARGETS), jnp.float32) * NUM_FEATURES ** -0.5
    w_star = jax.random.normal(sub_keys[7], (NUM_FEATURES, NUM_TARGETS), jnp.float32) * NUM_FEATURES ** -0.5
    targets = jnp.dot(design, w_star.astype(jnp.bfloat16), preferred_element_type=jnp.float32) + 0.3 * jax.random.normal(sub_keys[8], (NUM_ROWS, NUM_TARGETS), jnp.float32)
    return {"design": design, "targets": targets, "coef_init": coef_init, "step_sizes": step_sizes, "ridge_weights": ridge_weights}


def reference(design, targets, coef_init, step_sizes, ridge_weights):
    block_cols = NUM_FEATURES // FEAT_BLOCKS

    def block_sum(weights):
        weights_b = weights.astype(jnp.bfloat16)

        def add_block(acc_sum, block_index):
            col_block = lax.dynamic_slice_in_dim(design, block_index * block_cols, block_cols, 1)
            rows_w = lax.dynamic_slice_in_dim(weights_b, block_index * block_cols, block_cols, 0)
            product = jnp.dot(col_block, rows_w, preferred_element_type=jnp.float32)
            return acc_sum + product.astype(jnp.bfloat16).astype(jnp.float32), None

        return lax.scan(add_block, jnp.zeros((NUM_ROWS, NUM_TARGETS), jnp.float32), jnp.arange(FEAT_BLOCKS))[0]

    def sweep_once(sweep_state, unused):
        coef_cur, resid_cur = sweep_state
        gradient = lax.dot_general(design, resid_cur.astype(jnp.bfloat16), (((0,), (0,)), ((), ())), preferred_element_type=jnp.float32) / NUM_ROWS
        step_delta = step_sizes[:, None] * (gradient - ridge_weights[None, :] * coef_cur)
        return (coef_cur + STEP_WEIGHT * step_delta, resid_cur - STEP_WEIGHT * block_sum(step_delta)), None

    start_state = (coef_init, targets - block_sum(coef_init))
    final_state = lax.scan(sweep_once, start_state, None, length=SWEEPS)[0]
    return final_state[0], final_state[1]
```

```python
import functools

import jax
import jax.numpy as jnp
from jax import lax
from jax.experimental import pallas as pl
from jax.experimental.pallas import tpu as pltpu
from jax.sharding import PartitionSpec as P

SWEEPS = 4
STEP_WEIGHT = 0.5
CHUNK = 1024
SLOTS = 4
GROUPS = 2
MESH = pl.DeviceIdType.MESH


def sweep_kernel(
    total_rows, x_hbm, y_ref, w0_hbm, eta_ref, lam_ref, wt_hbm, rt_ref,
    xbuf, w0buf, gsend, grecv, ssend, srecv, wt, ut, rbt, uall,
    x_sem, w0_sem, g_send, g_recv, s_send, s_recv, u_send, u_recv, w_send, w_recv, out_sem,
):
    z, s, f = lax.axis_index("problem"), lax.axis_index("samp"), lax.axis_index("feat")
    chunks = wt.shape[0]
    targets = rt_ref.shape[0]
    per = targets // GROUPS
    core, chip = f % 2, f // 2
    near = chip * 2 + (1 - core)
    far = (1 - chip) * 2 + core
    partner_id = (z, 1 - s, f)
    near_id, far_id = (z, s, near), (z, s, far)
    own, other = s, 1 - s

    barrier = pltpu.get_barrier_semaphore()
    for device in (partner_id, near_id, far_id):
        pl.semaphore_signal(barrier, inc=1, device_id=device, device_id_type=MESH)

    def x_load(half, k):
        start = pl.multiple_of((half * chunks + k) * CHUNK, CHUNK)
        slot = k % SLOTS
        return pltpu.make_async_copy(x_hbm.at[:, pl.ds(start, CHUNK)], xbuf.at[slot], x_sem.at[slot])

    def w0_load(half, k):
        start = pl.multiple_of((half * chunks + k) * CHUNK, CHUNK)
        slot = k % SLOTS
        return pltpu.make_async_copy(w0_hbm.at[pl.ds(start, CHUNK), :], w0buf.at[slot], w0_sem.at[slot])

    def g_copy(g, k):
        return pltpu.make_async_remote_copy(
            src_ref=gsend.at[g, k], dst_ref=grecv.at[g, k], send_sem=g_send.at[g, k], recv_sem=g_recv.at[g, k],
            device_id=partner_id, device_id_type=MESH)

    def s_copy(g, k):
        return pltpu.make_async_remote_copy(
            src_ref=ssend.at[g, k], dst_ref=srecv.at[g, k], send_sem=s_send.at[g, k], recv_sem=s_recv.at[g, k],
            device_id=partner_id, device_id_type=MESH)

    def w_copy(half, k):
        return pltpu.make_async_remote_copy(
            src_ref=wt.at[k], dst_ref=wt_hbm.at[half * chunks + k], send_sem=w_send.at[k], recv_sem=w_recv.at[k],
            device_id=partner_id, device_id_type=MESH)

    def w_store(k):
        return pltpu.make_async_copy(wt.at[k], wt_hbm.at[own * chunks + k], out_sem.at[k])

    def u_copy(parity, g, slot, which, device):
        return pltpu.make_async_remote_copy(
            src_ref=uall.at[parity, g, slot], dst_ref=uall.at[parity, g, slot],
            send_sem=u_send.at[parity, g, which], recv_sem=u_recv.at[parity, g, which],
            device_id=device, device_id_type=MESH)

    def rows_of(g):
        return pl.ds(g * per, per)

    ahead = SLOTS - 1

    def steps(body, half, next_half=None, more=None):
        def step(k, carry):
            upcoming = k + ahead

            @pl.when(upcoming < chunks)
            def _():
                x_load(half, upcoming).start()

            if next_half is not None:
                wanted = upcoming >= chunks
                if more is not None:
                    wanted = jnp.logical_and(wanted, more)

                @pl.when(wanted)
                def _():
                    x_load(next_half, upcoming - chunks).start()

            x_load(half, k).wait()
            body(k, k % SLOTS)
            return carry

        lax.fori_loop(0, chunks, step, 0)

    for k in range(ahead):
        x_load(own, k).start()
        w0_load(own, k).start()
    ut[...] = jnp.zeros_like(ut)

    def start_half(half, next_half, keep):
        def body(k, slot):
            upcoming = k + ahead

            @pl.when(upcoming < chunks)
            def _():
                w0_load(half, upcoming).start()

            if keep:

                @pl.when(upcoming >= chunks)
                def _():
                    w0_load(next_half, upcoming - chunks).start()

            w0_load(half, k).wait()
            start_t = w0buf[slot].T
            if keep:
                wt[k] = start_t
            ut[...] += lax.dot_general(
                start_t.astype(jnp.bfloat16), xbuf[slot], (((1,), (1,)), ((), ())), preferred_element_type=jnp.float32)

        steps(body, half, next_half)

    start_half(own, other, True)
    rt_ref[...] = y_ref[...].T
    start_half(other, other, False)
    pl.semaphore_wait(barrier, 3)

    def u_begin(parity, g):
        uall[parity, g, f] = ut[rows_of(g), :].astype(jnp.bfloat16)
        ut[rows_of(g), :] = jnp.zeros((per, ut.shape[1]), jnp.float32)
        u_copy(parity, g, f, 0, near_id).start()
        u_copy(parity, g, f, 1, far_id).start()

    def u_end(parity, g, weight):
        u_copy(parity, g, far, 1, far_id).wait_recv()
        u_copy(parity, g, far, 2, near_id).start()
        u_copy(parity, g, near, 0, near_id).wait_recv()
        u_copy(parity, g, far, 2, near_id).wait_recv()
        total = uall[parity, g, 0].astype(jnp.float32)
        for block in range(1, 4):
            total += uall[parity, g, block].astype(jnp.float32)
        new = rt_ref[rows_of(g), :] - (total if weight is None else weight * total)
        rt_ref[rows_of(g), :] = new
        rbt[rows_of(g), :] = new.astype(jnp.bfloat16)
        u_copy(parity, g, f, 0, near_id).wait_send()
        u_copy(parity, g, f, 1, far_id).wait_send()
        u_copy(parity, g, far, 2, near_id).wait_send()

    def partner_gradient(g, next_half):
        def body(k, slot):
            @pl.when(k > 0)
            def _():
                g_copy(g, k - 1).start()

            gsend[g, k] = jnp.dot(rbt[rows_of(g), :], xbuf[slot], preferred_element_type=jnp.float32)

        steps(body, other, next_half)
        g_copy(g, chunks - 1).start()

    def own_columns(g, t, next_half):
        lam = lam_ref[rows_of(g), 0:1]

        def body(k, slot):
            part = jnp.dot(rbt[rows_of(g), :], xbuf[slot], preferred_element_type=jnp.float32)
            g_copy(g, k).wait_recv()

            @pl.when(t > 0)
            def _():
                s_copy(g, k).wait_send()

            weights = wt[k, rows_of(g), :]
            gradient = (part + grecv[g, k]) * (1.0 / total_rows)
            delta = eta_ref[pl.ds(own * chunks + k, 1), :] * (gradient - lam * weights)
            wt[k, rows_of(g), :] = weights + STEP_WEIGHT * delta
            delta_b = delta.astype(jnp.bfloat16)
            ssend[g, k] = delta_b
            ut[rows_of(g), :] += lax.dot_general(
                delta_b, xbuf[slot], (((1,), (1,)), ((), ())), preferred_element_type=jnp.float32)
            s_copy(g, k).start()

        steps(body, own, next_half)

    def partner_columns(g, next_half, more=None):
        def body(k, slot):
            s_copy(g, k).wait_recv()
            g_copy(g, k).wait_send()
            ut[rows_of(g), :] += lax.dot_general(
                srecv[g, k], xbuf[slot], (((1,), (1,)), ((), ())), preferred_element_type=jnp.float32)

        steps(body, other, next_half, more)

    u_begin(0, 0)
    u_begin(0, 1)
    u_end(0, 0, None)
    partner_gradient(0, other)
    u_end(0, 1, None)
    partner_gradient(1, own)

    def sweep(t, carry):
        parity = (t + 1) % 2
        more = t < SWEEPS - 1
        own_columns(0, t, own)
        own_columns(1, t, other)

        @pl.when(t == SWEEPS - 1)
        def _():
            def send(k, inner):
                w_copy(own, k).start()
                w_store(k).start()
                return inner

            lax.fori_loop(0, chunks, send, 0)

        partner_columns(0, other)
        u_begin(parity, 0)
        u_end(parity, 0, STEP_WEIGHT)

        @pl.when(more)
        def _():
            partner_gradient(0, other)

        partner_columns(1, other, more)
        u_begin(parity, 1)
        u_end(parity, 1, STEP_WEIGHT)

        @pl.when(more)
        def _():
            partner_gradient(1, own)

        return carry

    lax.fori_loop(0, SWEEPS, sweep, 0)

    def drain(k, carry):
        for g in range(GROUPS):
            s_copy(g, k).wait_send()
        w_store(k).wait()
        w_copy(own, k).wait_send()
        w_copy(other, k).wait_recv()
        return carry

    lax.fori_loop(0, chunks, drain, 0)


def finish_kernel(wt_ref, rt_ref, w_ref, r_ref):
    w_ref[...] = wt_ref[0].T

    @pl.when(pl.program_id(0) == 0)
    def _():
        r_ref[...] = rt_ref[...].T


def solution(mesh):
    samp_size = mesh.shape["samp"]
    design_spec = P(("problem", "samp"), "feat")
    rows_spec = P(("problem", "samp"), None)
    coef_spec = P(("problem", "feat"), None)
    step_spec = P(("problem", "feat"))
    ridge_spec = P("problem")

    def local_sweeps(design, targets, coef_init, step_sizes, ridge_weights):
        rows, columns = design.shape
        width = targets.shape[1]
        per = width // GROUPS
        chunks = columns // CHUNK // samp_size
        bf16, f32 = jnp.bfloat16, jnp.float32
        vmem, dma = pltpu.VMEM, pltpu.SemaphoreType.DMA
        in_vmem = pl.BlockSpec(memory_space=pltpu.VMEM)
        in_hbm = pl.BlockSpec(memory_space=pltpu.HBM)
        coef_t, resid_t = pl.pallas_call(
            functools.partial(sweep_kernel, rows * samp_size),
            name="sweeps",
            out_shape=(
                jax.ShapeDtypeStruct((columns // CHUNK, width, CHUNK), f32),
                jax.ShapeDtypeStruct((width, rows), f32),
            ),
            in_specs=[in_hbm, in_vmem, in_hbm, in_vmem, in_vmem],
            out_specs=(in_hbm, in_vmem),
            scratch_shapes=[
                vmem((SLOTS, rows, CHUNK), bf16),
                vmem((SLOTS, CHUNK, width), f32),
                vmem((GROUPS, chunks, per, CHUNK), f32),
                vmem((GROUPS, chunks, per, CHUNK), f32),
                vmem((GROUPS, chunks, per, CHUNK), bf16),
                vmem((GROUPS, chunks, per, CHUNK), bf16),
                vmem((chunks, width, CHUNK), f32),
                vmem((width, rows), f32),
                vmem((width, rows), bf16),
                vmem((2, GROUPS, 4, per, rows), bf16),
                dma((SLOTS,)),
                dma((SLOTS,)),
                dma((GROUPS, chunks)),
                dma((GROUPS, chunks)),
                dma((GROUPS, chunks)),
                dma((GROUPS, chunks)),
                dma((2, GROUPS, 3)),
                dma((2, GROUPS, 3)),
                dma((chunks,)),
                dma((chunks,)),
                dma((chunks,)),
            ],
            compiler_params=pltpu.CompilerParams(
                collective_id=0, has_side_effects=True, vmem_limit_bytes=67_000_000),
        )(
            design, targets, coef_init, step_sizes.reshape(columns // CHUNK, CHUNK),
            jnp.broadcast_to(ridge_weights[:, None], (width, 128)),
        )
        return pl.pallas_call(
            finish_kernel,
            name="finish",
            grid=(columns // CHUNK,),
            out_shape=(
                jax.ShapeDtypeStruct((columns, width), f32),
                jax.ShapeDtypeStruct((rows, width), f32),
            ),
            in_specs=[
                pl.BlockSpec((1, width, CHUNK), lambda i: (i, 0, 0)),
                pl.BlockSpec((width, rows), lambda i: (0, 0)),
            ],
            out_specs=(
                pl.BlockSpec((CHUNK, width), lambda i: (i, 0)),
                pl.BlockSpec((rows, width), lambda i: (0, 0)),
            ),
        )(coef_t, resid_t)

    return jax.shard_map(
        local_sweeps, mesh=mesh, in_specs=(design_spec, rows_spec, coef_spec, step_spec, ridge_spec),
        out_specs=(coef_spec, rows_spec), check_vma=False)
```

```python
import functools

import jax
import jax.numpy as jnp
from jax import lax
from jax.experimental import pallas as pl
from jax.experimental.pallas import tpu as pltpu
from jax.sharding import PartitionSpec as P

SWEEPS = 4
STEP_WEIGHT = 0.5
CHUNK = 1024
SLOTS = 4
GROUPS = ((0, 64), (64, 64))
KEPT = 4
PIECES = (6, 4, 2)
MESH = pl.DeviceIdType.MESH


def dot_t(left, right):
    return lax.dot_general(left, right, (((1,), (1,)), ((), ())), preferred_element_type=jnp.float32)


def sweep_kernel(
    total_rows, x_hbm, y_hbm, w0_hbm, eta_ref, lam_ref,
    r_hbm, w_near, w_far, *rest,
):
    w_pieces, rest = rest[: len(PIECES)], rest[len(PIECES):]
    (
        xbuf, w0buf, rows_buf, gsend, grecv, ssend, srecv, wt, ut, rt, rbt, uall, w0t_a, w0t_b, lam_col,
        x_sem, w0_sem, row_sem, g_send, g_recv, s_send, s_recv, u_send, u_recv, w_send, w_recv, out_sem,
    ) = rest
    z, s, f = lax.axis_index("problem"), lax.axis_index("samp"), lax.axis_index("feat")
    chunks, targets, _ = wt.shape
    core, chip = f % 2, f // 2
    near = chip * 2 + (1 - core)
    far = (1 - chip) * 2 + core
    partner_id = (z, 1 - s, f)
    near_id, far_id = (z, s, near), (z, s, far)
    own, other = s, 1 - s

    barrier = pltpu.get_barrier_semaphore()
    for device in (partner_id, near_id, far_id):
        pl.semaphore_signal(barrier, inc=1, device_id=device, device_id_type=MESH)

    def columns_of(chunk):
        return pl.ds(pl.multiple_of(chunk * CHUNK, CHUNK), CHUNK)

    def x_load(chunk, slot):
        return pltpu.make_async_copy(x_hbm.at[:, columns_of(chunk)], xbuf.at[slot], x_sem.at[slot])

    def w0_load(chunk, slot):
        return pltpu.make_async_copy(w0_hbm.at[columns_of(chunk), :], w0buf.at[slot], w0_sem.at[slot])

    def part(ref, g, k):
        return ref.at[k, pl.ds(*GROUPS[g]), :]

    def rows_of(g):
        return pl.ds(*GROUPS[g])

    def g_copy(g, k):
        return pltpu.make_async_remote_copy(
            src_ref=part(gsend, g, k), dst_ref=part(grecv, g, k), send_sem=g_send.at[g, k], recv_sem=g_recv.at[g, k],
            device_id=partner_id, device_id_type=MESH)

    def s_copy(g, k):
        return pltpu.make_async_remote_copy(
            src_ref=part(ssend, g, k), dst_ref=part(srecv, g, k), send_sem=s_send.at[g, k], recv_sem=s_recv.at[g, k],
            device_id=partner_id, device_id_type=MESH)

    def u_copy(parity, g, slot, which, device):
        rows = uall.at[parity, slot, rows_of(g), :]
        return pltpu.make_async_remote_copy(
            src_ref=rows, dst_ref=rows,
            send_sem=u_send.at[parity, g, which], recv_sem=u_recv.at[parity, g, which],
            device_id=device, device_id_type=MESH)

    ahead = SLOTS - 1

    def steps(body, half, next_half, more=None):
        def step(k, carry):
            upcoming = k + ahead

            @pl.when(upcoming < chunks)
            def _():
                x_load(half * chunks + upcoming, upcoming % SLOTS).start()

            wanted = upcoming >= chunks
            if more is not None:
                wanted = jnp.logical_and(wanted, more)

            @pl.when(wanted)
            def _():
                x_load(next_half * chunks + upcoming - chunks, upcoming % SLOTS).start()

            x_load(half * chunks + k, k % SLOTS).wait()
            body(k, k % SLOTS)
            return carry

        lax.fori_loop(0, chunks, step, 0)

    y_load = pltpu.make_async_copy(y_hbm, rows_buf, row_sem)
    w0_load(0, 0).start()
    for k in range(ahead):
        x_load(k, k).start()
        w0_load(k + 1, (k + 1) % SLOTS).start()
    y_load.start()
    ut[...] = jnp.zeros_like(ut)
    lam_col[...] = jnp.broadcast_to(lam_ref[0:1, :], (targets, targets)).T
    w0_load(0, 0).wait()
    w0t_a[...] = w0buf[0].T.astype(jnp.bfloat16)
    w0_load(4, 0).start()
    y_load.wait()
    rt[...] = rows_buf[...].T
    blocks = 2 * chunks

    def start_pair(pair, carry):
        for odd in range(2):
            now, later = (w0t_b, w0t_a) if odd else (w0t_a, w0t_b)
            chunk = pair * 2 + odd
            slot = chunk % SLOTS
            upcoming = chunk + ahead

            @pl.when(upcoming < blocks)
            def _():
                x_load(upcoming, upcoming % SLOTS).start()

            @pl.when(upcoming >= blocks)
            def _():
                x_load(other * chunks + upcoming - blocks, upcoming % SLOTS).start()

            following = (chunk + 1) % blocks
            w0_load(following, (chunk + 1) % SLOTS).wait()
            x_load(chunk, slot).wait()
            later[...] = w0buf[(chunk + 1) % SLOTS].T.astype(jnp.bfloat16)
            ut[...] += dot_t(now[...], xbuf[slot])
            w0_load((chunk + 5) % blocks, (chunk + 1) % SLOTS).start()
        return carry

    lax.fori_loop(0, chunks, start_pair, 0)
    for k in range(1, 5):
        w0_load(k, k % SLOTS).wait()
    pl.semaphore_wait(barrier, 3)

    def u_begin(parity, g):
        uall[parity, f, rows_of(g), :] = ut[rows_of(g), :].astype(jnp.bfloat16)
        ut[rows_of(g), :] = jnp.zeros((GROUPS[g][1], ut.shape[1]), jnp.float32)
        u_copy(parity, g, f, 0, near_id).start()
        u_copy(parity, g, f, 1, far_id).start()

    def u_end(parity, g, weight):
        u_copy(parity, g, far, 1, far_id).wait_recv()
        u_copy(parity, g, far, 2, near_id).start()
        u_copy(parity, g, near, 0, near_id).wait_recv()
        u_copy(parity, g, far, 2, near_id).wait_recv()
        total = uall[parity, 0, rows_of(g), :].astype(jnp.float32)
        for block in range(1, 4):
            total += uall[parity, block, rows_of(g), :].astype(jnp.float32)
        new = rt[rows_of(g), :] - (total if weight is None else weight * total)
        rt[rows_of(g), :] = new
        rbt[rows_of(g), :] = new.astype(jnp.bfloat16)
        u_copy(parity, g, f, 0, near_id).wait_send()
        u_copy(parity, g, f, 1, far_id).wait_send()
        u_copy(parity, g, far, 2, near_id).wait_send()

    def partner_gradient(g, next_half):
        def body(k, slot):
            @pl.when(k > 0)
            def _():
                g_copy(g, k - 1).start()

            gsend[k, rows_of(g), :] = jnp.dot(rbt[rows_of(g), :], xbuf[slot], preferred_element_type=jnp.float32)

        steps(body, other, next_half)
        g_copy(g, chunks - 1).start()

    def own_columns(g, t, next_half):
        lam = lam_col[rows_of(g), 0:1]

        def body(k, slot):
            mine = jnp.dot(rbt[rows_of(g), :], xbuf[slot], preferred_element_type=jnp.float32)
            g_copy(g, k).wait_recv()

            @pl.when(t > 0)
            def _():
                s_copy(g, k).wait_send()

            weights = wt[k, rows_of(g), :]
            gradient = (mine + grecv[k, rows_of(g), :]) * (1.0 / total_rows)
            delta = eta_ref[0:1, columns_of(own * chunks + k)] * (gradient - lam * weights)
            wt[k, rows_of(g), :] = weights + STEP_WEIGHT * delta
            delta_b = delta.astype(jnp.bfloat16)
            ssend[k, rows_of(g), :] = delta_b
            ut[rows_of(g), :] += dot_t(delta_b, xbuf[slot])
            s_copy(g, k).start()

        steps(body, own, next_half)

    def partner_columns(g, next_half, more=None):
        def body(k, slot):
            s_copy(g, k).wait_recv()
            g_copy(g, k).wait_send()
            ut[rows_of(g), :] += dot_t(srecv[k, rows_of(g), :], xbuf[slot])

        steps(body, other, next_half, more)

    u_begin(0, 0)
    u_begin(0, 1)
    u_end(0, 0, None)
    partner_gradient(0, other)
    u_end(0, 1, None)
    partner_gradient(1, own)

    for k in range(ahead):
        w0_load(own * chunks + k, k).start()

    def keep(k, carry):
        @pl.when(k + ahead < chunks)
        def _():
            w0_load(own * chunks + k + ahead, (k + ahead) % SLOTS).start()

        w0_load(own * chunks + k, k % SLOTS).wait()
        wt[k] = w0buf[k % SLOTS].T
        return carry

    lax.fori_loop(0, chunks, keep, 0)

    def w_store(ref, first, n, k):
        rows = pl.ds(pl.multiple_of(k * CHUNK, CHUNK), CHUNK)
        slot = (first + k) % SLOTS
        return pltpu.make_async_copy(w0buf.at[slot], ref.at[rows, :], out_sem.at[slot])

    def w_copy(k):
        rows = pl.ds(pl.multiple_of(k * CHUNK, CHUNK), CHUNK)
        slot = k % SLOTS
        return pltpu.make_async_remote_copy(
            src_ref=w0buf.at[slot], dst_ref=w_far.at[rows, :], send_sem=w_send.at[slot], recv_sem=w_recv.at[slot],
            device_id=partner_id, device_id_type=MESH)

    def w_out():
        first = 0
        for ref, n in (*zip(w_pieces, PIECES), (w_near, KEPT)):

            def put(k, carry, ref=ref, n=n, first=first):
                chunk = first + k
                slot = chunk % SLOTS

                @pl.when(chunk >= SLOTS)
                def _():
                    w_store(ref, first, n, k).wait()

                w0buf[slot] = wt[chunk].T
                w_store(ref, first, n, k).start()
                return carry

            lax.fori_loop(0, n, put, 0)
            first += n

        def send(k, carry):
            w_copy(k).start()
            return carry

        lax.fori_loop(0, KEPT, send, 0)

    def sweep(t, carry):
        parity = (t + 1) % 2
        more = t < SWEEPS - 1
        own_columns(0, t, own)
        own_columns(1, t, other)

        @pl.when(jnp.logical_not(more))
        def _():
            w_out()

        partner_columns(0, other)
        u_begin(parity, 0)
        u_end(parity, 0, STEP_WEIGHT)

        @pl.when(more)
        def _():
            partner_gradient(0, other)

        partner_columns(1, other, more)
        u_begin(parity, 1)
        u_end(parity, 1, STEP_WEIGHT)

        @pl.when(more)
        def _():
            partner_gradient(1, own)

        return carry

    lax.fori_loop(0, SWEEPS, sweep, 0)
    rows_buf[...] = rt[...].T
    r_store = pltpu.make_async_copy(rows_buf, r_hbm, row_sem)
    r_store.start()

    def drain(k, carry):
        for g in range(len(GROUPS)):
            s_copy(g, k).wait_send()
        return carry

    lax.fori_loop(0, chunks, drain, 0)
    for k in range(KEPT):
        w_store(w_near, sum(PIECES), KEPT, k).wait()
        w_copy(k).wait()
    r_store.wait()


def place(result, piece, half, first, shape):
    rows, width = piece.shape
    halves = shape[0] // CHUNK // 2

    def body(half_ref, piece_ref, *refs):
        refs[-1][...] = piece_ref[...]

    in_specs = [pl.BlockSpec((CHUNK, width), lambda i, half_ref: (i, 0))]
    operands = [piece]
    aliases = {}
    if result is not None:
        in_specs.append(pl.BlockSpec(memory_space=pl.ANY))
        operands.append(result)
        aliases = {2: 0}
    return pl.pallas_call(
        body,
        name="place",
        out_shape=jax.ShapeDtypeStruct(shape, piece.dtype),
        grid_spec=pltpu.PrefetchScalarGridSpec(
            num_scalar_prefetch=1,
            grid=(rows // CHUNK,),
            in_specs=in_specs,
            out_specs=pl.BlockSpec((CHUNK, width), lambda i, half_ref: (half_ref[0] * halves + first + i, 0)),
        ),
        input_output_aliases=aliases,
    )(half, *operands)


def solution(mesh):
    samp_size = mesh.shape["samp"]
    design_spec = P(("problem", "samp"), "feat")
    rows_spec = P(("problem", "samp"), None)
    coef_spec = P(("problem", "feat"), None)
    step_spec = P(("problem", "feat"))
    ridge_spec = P("problem")

    def local_sweeps(design, targets, coef_init, step_sizes, ridge_weights):
        rows, columns = design.shape
        width = targets.shape[1]
        groups = len(GROUPS)
        chunks = columns // CHUNK // samp_size
        bf16, f32 = jnp.bfloat16, jnp.float32
        vmem, dma = pltpu.VMEM, pltpu.SemaphoreType.DMA
        in_vmem = pl.BlockSpec(memory_space=pltpu.VMEM)
        in_hbm = pl.BlockSpec(memory_space=pltpu.HBM)
        sizes = (KEPT, KEPT, *PIECES)
        resid, near, far, *pieces = pl.pallas_call(
            functools.partial(sweep_kernel, rows * samp_size),
            name="sweeps",
            out_shape=(
                jax.ShapeDtypeStruct((rows, width), f32),
                *(jax.ShapeDtypeStruct((n * CHUNK, width), f32) for n in sizes),
            ),
            in_specs=[in_hbm, in_hbm, in_hbm, in_vmem, in_vmem],
            out_specs=(in_hbm,) * (1 + len(sizes)),
            scratch_shapes=[
                vmem((SLOTS, rows, CHUNK), bf16),
                vmem((SLOTS, CHUNK, width), f32),
                vmem((rows, width), f32),
                vmem((chunks, width, CHUNK), f32),
                vmem((chunks, width, CHUNK), f32),
                vmem((chunks, width, CHUNK), bf16),
                vmem((chunks, width, CHUNK), bf16),
                vmem((chunks, width, CHUNK), f32),
                vmem((width, rows), f32),
                vmem((width, rows), f32),
                vmem((width, rows), bf16),
                vmem((2, 4, width, rows), bf16),
                vmem((width, CHUNK), bf16),
                vmem((width, CHUNK), bf16),
                vmem((width, width), f32),
                dma((SLOTS,)),
                dma((SLOTS,)),
                dma,
                dma((groups, chunks)),
                dma((groups, chunks)),
                dma((groups, chunks)),
                dma((groups, chunks)),
                dma((2, groups, 3)),
                dma((2, groups, 3)),
                dma((SLOTS,)),
                dma((SLOTS,)),
                dma((SLOTS,)),
            ],
            compiler_params=pltpu.CompilerParams(
                collective_id=0, has_side_effects=True, vmem_limit_bytes=67_000_000),
        )(design, targets, coef_init, step_sizes.reshape(1, columns), ridge_weights.reshape(1, width))
        here = lax.axis_index("samp").astype(jnp.int32).reshape(1)
        swap = [(i, samp_size - 1 - i) for i in range(samp_size)]
        arrived = [lax.ppermute(piece, "samp", swap) for piece in pieces]
        shape = (columns, width)
        coef = place(None, near, here, sum(PIECES), shape)
        first = 0
        for piece, n in zip(pieces, PIECES):
            coef = place(coef, piece, here, first, shape)
            first += n
        coef = place(coef, far, 1 - here, sum(PIECES), shape)
        first = 0
        for piece, n in zip(arrived, PIECES):
            coef = place(coef, piece, 1 - here, first, shape)
            first += n
        return coef, resid

    return jax.shard_map(
        local_sweeps, mesh=mesh, in_specs=(design_spec, rows_spec, coef_spec, step_spec, ridge_spec),
        out_specs=(coef_spec, rows_spec), check_vma=False)
```

```python
import functools

import jax
import jax.numpy as jnp
from jax import lax
from jax.experimental import pallas as pl
from jax.experimental.pallas import tpu as pltpu
from jax.sharding import PartitionSpec as P

SWEEPS = 4
STEP_WEIGHT = 0.5
CHUNK = 1024
SLOTS = 4
GROUPS = ((0, 64), (64, 64))
SHIPPED = 640
ROW_BLOCKS = 4
KEPT = 4
PIECES = (6, 5, 1)
MESH = pl.DeviceIdType.MESH


def dot_t(left, right):
    return lax.dot_general(left, right, (((1,), (1,)), ((), ())), preferred_element_type=jnp.float32)


def sweep_kernel(
    total_rows, x_hbm, y_hbm, w0_hbm, eta_hbm, lam_hbm,
    r_hbm, shipped_hbm, w_near, w_far, *rest,
):
    w_pieces, rest = rest[: len(PIECES)], rest[len(PIECES):]
    (
        xbuf, w0buf, gsend, grecv, sbuf, wt, ut, acc, rt, rbt, ra, uall, eta_ref, lam_ref, lam_col,
        x_sem, w0_sem, in_sem, ship_sem, r_send, r_recv, g_send, g_recv, s_send, s_recv, f_send, f_recv, u_send, u_recv, w_send, w_recv, out_sem,
    ) = rest
    z, s, f = lax.axis_index("problem"), lax.axis_index("samp"), lax.axis_index("feat")
    chunks, targets, _ = wt.shape
    core, chip = f % 2, f // 2
    near = chip * 2 + (1 - core)
    far = (1 - chip) * 2 + core
    partner_id = (z, 1 - s, f)
    near_id, far_id = (z, s, near), (z, s, far)
    own, other = s, 1 - s

    barrier = pltpu.get_barrier_semaphore()
    for device in (partner_id, near_id, far_id):
        pl.semaphore_signal(barrier, inc=1, device_id=device, device_id_type=MESH)

    def columns_of(chunk):
        return pl.ds(pl.multiple_of(chunk * CHUNK, CHUNK), CHUNK)

    def x_load(chunk, slot):
        return pltpu.make_async_copy(x_hbm.at[:, columns_of(chunk)], xbuf.at[slot], x_sem.at[slot, 0])

    def w0_load(chunk, slot):
        return pltpu.make_async_copy(w0_hbm.at[columns_of(chunk), :], w0buf.at[slot], w0_sem.at[slot])

    def part(ref, g, k):
        return ref.at[k, pl.ds(*GROUPS[g]), :]

    def rows_of(g):
        return pl.ds(*GROUPS[g])

    def g_copy(g, k):
        return pltpu.make_async_remote_copy(
            src_ref=part(gsend, g, k), dst_ref=part(grecv, g, k), send_sem=g_send.at[g, k], recv_sem=g_recv.at[g, k],
            device_id=partner_id, device_id_type=MESH)

    def s_copy(g, k):
        return pltpu.make_async_remote_copy(
            src_ref=part(sbuf, g, k), dst_ref=part(sbuf, g, chunks + k), send_sem=s_send.at[g, k], recv_sem=s_recv.at[g, k],
            device_id=partner_id, device_id_type=MESH)

    def u_copy(parity, g, slot, which, device):
        rows = uall.at[parity, slot, rows_of(g), :]
        return pltpu.make_async_remote_copy(
            src_ref=rows, dst_ref=rows,
            send_sem=u_send.at[parity, g, which], recv_sem=u_recv.at[parity, g, which],
            device_id=device, device_id_type=MESH)

    ahead = SLOTS - 1

    def start(copy):
        copy.start(priority=1)

    def wait(copy):
        copy.wait()

    def other_load(i, slot, act):
        act(x_load(other * chunks + i, slot))

    def own_load(i, slot, act):
        @pl.when(i != chunks - 1)
        def _():
            act(x_load(own * chunks + i - i // chunks, slot))

        @pl.when(i == chunks - 1)
        def _():
            act(pltpu.make_async_copy(shipped_hbm, xbuf.at[slot, :, pl.ds(0, SHIPPED)], x_sem.at[slot, 0]))

    def steps(base, count, load, next_load, body, more=None):
        def step(i, carry):
            upcoming = i + ahead
            slot = (base + upcoming) % SLOTS

            @pl.when(upcoming < count)
            def _():
                load(upcoming, slot, start)

            wanted = upcoming >= count
            if more is not None:
                wanted = jnp.logical_and(wanted, more)

            @pl.when(wanted)
            def _():
                next_load(upcoming - count, slot, start)

            load(i, (base + i) % SLOTS, wait)
            body(i, (base + i) % SLOTS)
            return carry

        lax.fori_loop(0, count, step, 0)

    rows = x_hbm.shape[0] // ROW_BLOCKS
    width = xbuf.shape[1] // rows
    passes = 2 * chunks // width
    blocks = ROW_BLOCKS * passes
    pairs = w0buf.shape[0] // 2

    def tile_load(step, q):
        slot = step % SLOTS
        where = pl.ds(pl.multiple_of(step // passes * rows, rows), rows)
        return pltpu.make_async_copy(
            x_hbm.at[where, columns_of(step % passes * width + q)], xbuf.at[slot, pl.ds(q * rows, rows), :], x_sem.at[slot, q])

    def tiles_ahead(step):
        upcoming = step + ahead

        @pl.when(upcoming < blocks)
        def _():
            for q in range(width):
                tile_load(upcoming, q).start(priority=1)

        @pl.when(upcoming >= blocks)
        def _():
            x_load(other * chunks + upcoming - blocks, upcoming % SLOTS).start(priority=1)

    def w0_pair(pair, q):
        return w0_load(2 * pair + q, 2 * (pair % pairs) + q)

    eta_load = pltpu.make_async_copy(eta_hbm, eta_ref, in_sem.at[0])
    lam_load = pltpu.make_async_copy(lam_hbm, lam_ref, in_sem.at[1])
    halves = [
        pltpu.make_async_copy(
            y_hbm.at[pl.ds(i * CHUNK, CHUNK), :], w0buf.at[2 * pairs - 2 + i], w0_sem.at[2 * pairs - 2 + i])
        for i in range(2)
    ]
    for load in (*halves, lam_load, eta_load):
        load.start()
    for pair in range(pairs - 1):
        for q in range(2):
            w0_pair(pair, q).start()
    for step in range(ahead):
        for q in range(width):
            tile_load(step, q).start(priority=1)
    ut[...] = jnp.zeros_like(ut)
    acc[...] = jnp.zeros_like(acc)
    for i, load in enumerate(halves):
        load.wait()
        rt[:, i * CHUNK:(i + 1) * CHUNK] = w0buf[2 * pairs - 2 + i].T
    pl.semaphore_wait(barrier, 3)
    ship = pltpu.make_async_remote_copy(
        src_ref=x_hbm.at[:, pl.ds(pl.multiple_of((other + 1) * chunks * CHUNK - SHIPPED, 128), SHIPPED)],
        dst_ref=shipped_hbm, send_sem=ship_sem.at[0], recv_sem=ship_sem.at[1],
        device_id=partner_id, device_id_type=MESH)
    ship.start()
    lam_load.wait()
    lam_col[...] = jnp.broadcast_to(lam_ref[0:1, :], (targets, targets)).T

    def first_pass(pair, carry):
        @pl.when(pair % (width // 2) == 0)
        def _():
            tiles_ahead(pair // (width // 2))

        @pl.when(pair + pairs - 1 < chunks)
        def _():
            for q in range(2):
                w0_pair(pair + pairs - 1, q).start()

        slot = pair // (width // 2) % SLOTS
        first = pair % (width // 2) * 2
        total = acc[...]
        for q in range(2):
            w0_pair(pair, q).wait()
            tile_load(pair // (width // 2), first + q).wait()
        for q in range(2):
            turned = w0buf[2 * (pair % pairs) + q].T.astype(jnp.bfloat16)
            sbuf[2 * pair + q] = turned
            where = pl.ds(pl.multiple_of((first + q) * rows, rows), rows)
            total += dot_t(turned, xbuf[slot, where, :])
        acc[...] = total
        return carry

    def later_pass(block, carry):
        def step_(i, inner):
            step = block * passes + i
            tiles_ahead(step)
            for q in range(width):
                tile_load(step, q).wait()
            slot = step % SLOTS
            total = acc[...]
            for q in range(width):
                total += dot_t(sbuf[i * width + q], xbuf[slot, q * rows:(q + 1) * rows, :])
            acc[...] = total
            return inner

        lax.fori_loop(0, passes, step_, 0)
        return carry

    def lanes_of(block):
        return pl.ds(block * rows, rows)

    def first_copy(block, g, slot, which, device):
        ref = uall.at[0, slot, rows_of(g), lanes_of(block)]
        return pltpu.make_async_remote_copy(
            src_ref=ref, dst_ref=ref, send_sem=f_send.at[block, g, which], recv_sem=f_recv.at[block, g, which],
            device_id=device, device_id_type=MESH)

    def first_begin(block):
        uall[0, f, :, lanes_of(block)] = acc[...].astype(jnp.bfloat16)
        acc[...] = jnp.zeros_like(acc)
        for g in range(len(GROUPS)):
            first_copy(block, g, f, 0, near_id).start()
            first_copy(block, g, f, 1, far_id).start()

    def first_forward(block, g):
        first_copy(block, g, far, 1, far_id).wait_recv()
        first_copy(block, g, far, 2, near_id).start()

    def first_end(block, g):
        first_copy(block, g, near, 0, near_id).wait_recv()
        first_copy(block, g, far, 2, near_id).wait_recv()
        total = uall[0, 0, rows_of(g), lanes_of(block)].astype(jnp.float32)
        for j in range(1, 4):
            total += uall[0, j, rows_of(g), lanes_of(block)].astype(jnp.float32)
        new = rt[rows_of(g), lanes_of(block)] - total
        rt[rows_of(g), lanes_of(block)] = new
        rbt[rows_of(g), lanes_of(block)] = new.astype(jnp.bfloat16)
        first_copy(block, g, f, 0, near_id).wait_send()
        first_copy(block, g, f, 1, far_id).wait_send()
        first_copy(block, g, far, 2, near_id).wait_send()

    lax.fori_loop(0, chunks, first_pass, 0)
    last = ROW_BLOCKS - 1
    for block in range(ROW_BLOCKS):
        if block:
            later_pass(block, 0)
        first_begin(block)
        for g in range(len(GROUPS)):
            if block >= 1:
                first_forward(block - 1, g)
            if block >= 2:
                first_end(block - 2, g)

    def u_begin(parity, g):
        uall[parity, f, rows_of(g), :] = ut[rows_of(g), :].astype(jnp.bfloat16)
        ut[rows_of(g), :] = jnp.zeros((GROUPS[g][1], ut.shape[1]), jnp.float32)
        u_copy(parity, g, f, 0, near_id).start()
        u_copy(parity, g, f, 1, far_id).start()

    def u_end(parity, g):
        u_copy(parity, g, far, 1, far_id).wait_recv()
        u_copy(parity, g, far, 2, near_id).start()
        u_copy(parity, g, near, 0, near_id).wait_recv()
        u_copy(parity, g, far, 2, near_id).wait_recv()
        total = uall[parity, 0, rows_of(g), :].astype(jnp.float32)
        for block in range(1, 4):
            total += uall[parity, block, rows_of(g), :].astype(jnp.float32)
        new = rt[rows_of(g), :] - STEP_WEIGHT * total
        rt[rows_of(g), :] = new
        rbt[rows_of(g), :] = new.astype(jnp.bfloat16)
        u_copy(parity, g, f, 0, near_id).wait_send()
        u_copy(parity, g, f, 1, far_id).wait_send()
        u_copy(parity, g, far, 2, near_id).wait_send()

    quarter = ra.shape[1] // 4

    def r_copy(g, source, of, which, device):
        lanes = pl.ds(pl.multiple_of(of * quarter, quarter), quarter)
        return pltpu.make_async_remote_copy(
            src_ref=source.at[rows_of(g), lanes], dst_ref=ra.at[rows_of(g), lanes],
            send_sem=r_send.at[g, which], recv_sem=r_recv.at[g, which], device_id=device, device_id_type=MESH)

    def r_begin(g):
        r_copy(g, rbt, f, 0, partner_id).start()

    def r_spread(g):
        r_copy(g, rbt, f, 0, partner_id).wait()
        r_copy(g, ra, f, 1, near_id).start()
        r_copy(g, ra, f, 2, far_id).start()

    def r_end(g):
        r_copy(g, ra, far, 2, far_id).wait_recv()
        r_copy(g, ra, far, 3, near_id).start()
        r_copy(g, ra, near, 1, near_id).wait_recv()
        r_copy(g, ra, far, 3, near_id).wait_recv()
        r_copy(g, ra, f, 1, near_id).wait_send()
        r_copy(g, ra, f, 2, far_id).wait_send()
        r_copy(g, ra, far, 3, near_id).wait_send()

    sent = CHUNK - SHIPPED

    def last_copy(g):
        lanes = pl.ds(0, sent)
        return pltpu.make_async_remote_copy(
            src_ref=gsend.at[chunks - 1, rows_of(g), lanes], dst_ref=grecv.at[chunks - 1, rows_of(g), lanes],
            send_sem=g_send.at[g, chunks - 1], recv_sem=g_recv.at[g, chunks - 1],
            device_id=partner_id, device_id_type=MESH)

    def for_g_copy(g, k, act):
        @pl.when(k < chunks - 1)
        def _():
            act(g_copy(g, k))

        @pl.when(k == chunks - 1)
        def _():
            act(last_copy(g))

    def partner_gradient(g, base, next_load):
        def body(k, slot):
            @pl.when(k > 0)
            def _():
                g_copy(g, k - 1).start()

            gsend[k, rows_of(g), :] = jnp.dot(rbt[rows_of(g), :], xbuf[slot], preferred_element_type=jnp.float32)

        steps(base, chunks, other_load, next_load, body)
        last_copy(g).start()

    def own_columns(g, t, base, next_load):
        lam = lam_col[rows_of(g), 0:1]

        def body(i, slot):
            @pl.when(i == chunks - 1)
            def _():
                r_end(g)
                grecv[chunks - 1, rows_of(g), sent:] = jnp.dot(
                    ra[rows_of(g), :], xbuf[slot, :, 0:SHIPPED], preferred_element_type=jnp.float32)

            @pl.when(i != chunks - 1)
            def _():
                k = i - i // chunks
                for_g_copy(g, k, lambda copy: copy.wait_recv())

                @pl.when(t > 0)
                def _():
                    s_copy(g, k).wait_send()

                mine = jnp.dot(rbt[rows_of(g), :], xbuf[slot], preferred_element_type=jnp.float32)
                weights = wt[k, rows_of(g), :]
                gradient = (mine + grecv[k, rows_of(g), :]) * (1.0 / total_rows)
                lanes = eta_ref.shape[1]
                first = (own * chunks + k) * (CHUNK // lanes)
                eta = jnp.concatenate([eta_ref[pl.ds(first + j, 1), :] for j in range(CHUNK // lanes)], axis=1)
                delta = eta * (gradient - lam * weights)
                wt[k, rows_of(g), :] = weights + STEP_WEIGHT * delta
                delta_b = delta.astype(jnp.bfloat16)
                sbuf[k, rows_of(g), :] = delta_b
                ut[rows_of(g), :] += dot_t(delta_b, xbuf[slot])
                s_copy(g, k).start()

        steps(base, chunks + 1, own_load, next_load, body)

    def partner_columns(g, base, next_load, more=None):
        def body(k, slot):
            s_copy(g, k).wait_recv()
            for_g_copy(g, k, lambda copy: copy.wait_send())
            ut[rows_of(g), :] += dot_t(sbuf[chunks + k, rows_of(g), :], xbuf[slot])

        steps(base, chunks, other_load, next_load, body, more)

    first_forward(last, 0)
    first_end(last - 1, 0)
    first_end(last, 0)
    r_begin(0)
    first_forward(last, 1)
    partner_gradient(0, blocks, other_load)
    first_end(last - 1, 1)
    first_end(last, 1)
    r_begin(1)
    partner_gradient(1, blocks, own_load)

    eta_load.wait()
    for k in range(ahead):
        w0_load(own * chunks + k, k).start()

    def keep(k, carry):
        @pl.when(k + ahead < chunks)
        def _():
            w0_load(own * chunks + k + ahead, (k + ahead) % SLOTS).start()

        w0_load(own * chunks + k, k % SLOTS).wait()
        wt[k] = w0buf[k % SLOTS].T
        return carry

    lax.fori_loop(0, chunks, keep, 0)
    ship.wait()
    r_spread(0)

    def w_store(ref, first, n, k):
        rows = pl.ds(pl.multiple_of(k * CHUNK, CHUNK), CHUNK)
        slot = (first + k) % SLOTS
        return pltpu.make_async_copy(w0buf.at[slot], ref.at[rows, :], out_sem.at[slot])

    def w_copy(k):
        rows = pl.ds(pl.multiple_of(k * CHUNK, CHUNK), CHUNK)
        slot = k % SLOTS
        return pltpu.make_async_remote_copy(
            src_ref=w0buf.at[slot], dst_ref=w_far.at[rows, :], send_sem=w_send.at[slot], recv_sem=w_recv.at[slot],
            device_id=partner_id, device_id_type=MESH)

    def w_out():
        first = 0
        for ref, n in (*zip(w_pieces, PIECES), (w_near, KEPT)):

            def put(k, carry, ref=ref, n=n, first=first):
                chunk = first + k
                slot = chunk % SLOTS

                @pl.when(chunk >= SLOTS)
                def _():
                    w_store(ref, first, n, k).wait()

                w0buf[slot] = wt[chunk].T
                w_store(ref, first, n, k).start()
                return carry

            lax.fori_loop(0, n, put, 0)
            first += n

        def send(k, carry):
            w_copy(k).start()
            return carry

        lax.fori_loop(0, KEPT, send, 0)

    def sweep(t, carry):
        parity = (t + 1) % 2
        more = t < SWEEPS - 1
        at = t * (6 * chunks + 2)
        own_columns(0, t, at, own_load)
        r_spread(1)
        own_columns(1, t, at + chunks + 1, other_load)

        @pl.when(jnp.logical_not(more))
        def _():
            w_out()

        at = at + 2 * chunks + 2
        partner_columns(0, at, other_load)
        u_begin(parity, 0)
        u_end(parity, 0)

        @pl.when(more)
        def _():
            r_begin(0)
            partner_gradient(0, at, other_load)

        partner_columns(1, at, other_load, more)

        @pl.when(more)
        def _():
            r_spread(0)

        u_begin(parity, 1)
        u_end(parity, 1)

        @pl.when(more)
        def _():
            r_begin(1)
            partner_gradient(1, at, own_load)

        return carry

    lax.fori_loop(0, SWEEPS, sweep, 0)
    r_stores = []
    for i in range(2):
        w0buf[SLOTS + i] = rt[:, i * CHUNK:(i + 1) * CHUNK].T
        r_stores.append(
            pltpu.make_async_copy(w0buf.at[SLOTS + i], r_hbm.at[pl.ds(i * CHUNK, CHUNK), :], in_sem.at[i]))
        r_stores[i].start()

    def drain(k, carry):
        for g in range(len(GROUPS)):
            s_copy(g, k).wait_send()
        return carry

    lax.fori_loop(0, chunks, drain, 0)
    for k in range(KEPT):
        w_store(w_near, sum(PIECES), KEPT, k).wait()
        w_copy(k).wait()
    for store in r_stores:
        store.wait()


def place(result, piece, half, first, shape, extra=None):
    rows, width = piece.shape
    halves = shape[0] // CHUNK // 2
    here = pl.BlockSpec((CHUNK, width), lambda i, half_ref: (half_ref[0] * halves + first + i, 0))
    out_shape, out_specs = [jax.ShapeDtypeStruct(shape, piece.dtype)], [here]

    def body(half_ref, piece_ref, other_ref, out_ref, *copied):
        out_ref[...] = piece_ref[...]
        for ref in copied:
            ref[...] = other_ref[...]

    if result is None:
        whole = pl.BlockSpec(extra.shape, lambda i, half_ref: (0, 0))
        out_shape.append(jax.ShapeDtypeStruct(extra.shape, extra.dtype))
        out_specs.append(whole)
        other, other_spec, aliases = extra, whole, {}
    else:
        other, other_spec, aliases = result, pl.BlockSpec(memory_space=pl.ANY), {2: 0}
    return pl.pallas_call(
        body,
        name="place",
        out_shape=out_shape,
        grid_spec=pltpu.PrefetchScalarGridSpec(
            num_scalar_prefetch=1,
            grid=(rows // CHUNK,),
            in_specs=[pl.BlockSpec((CHUNK, width), lambda i, half_ref: (i, 0)), other_spec],
            out_specs=out_specs,
        ),
        input_output_aliases=aliases,
    )(half, piece, other)


def solution(mesh):
    samp_size = mesh.shape["samp"]
    design_spec = P(("problem", "samp"), "feat")
    rows_spec = P(("problem", "samp"), None)
    coef_spec = P(("problem", "feat"), None)
    step_spec = P(("problem", "feat"))
    ridge_spec = P("problem")

    def local_sweeps(design, targets, coef_init, step_sizes, ridge_weights):
        rows, columns = design.shape
        width = targets.shape[1]
        groups = len(GROUPS)
        chunks = columns // CHUNK // samp_size
        bf16, f32 = jnp.bfloat16, jnp.float32
        vmem, dma = pltpu.VMEM, pltpu.SemaphoreType.DMA
        in_hbm = pl.BlockSpec(memory_space=pltpu.HBM)
        sizes = (KEPT, KEPT, *PIECES)
        resid, _, near, far, *pieces = pl.pallas_call(
            functools.partial(sweep_kernel, rows * samp_size),
            name="sweeps",
            out_shape=(
                jax.ShapeDtypeStruct((rows, width), f32),
                jax.ShapeDtypeStruct((rows, SHIPPED), bf16),
                *(jax.ShapeDtypeStruct((n * CHUNK, width), f32) for n in sizes),
            ),
            in_specs=[in_hbm] * 5,
            out_specs=(in_hbm,) * (2 + len(sizes)),
            scratch_shapes=[
                vmem((SLOTS, rows, CHUNK), bf16),
                vmem((SLOTS + 2, CHUNK, width), f32),
                vmem((chunks, width, CHUNK), f32),
                vmem((chunks, width, CHUNK), f32),
                vmem((2 * chunks, width, CHUNK), bf16),
                vmem((chunks, width, CHUNK), f32),
                vmem((width, rows), f32),
                vmem((width, rows // ROW_BLOCKS), f32),
                vmem((width, rows), f32),
                vmem((width, rows), bf16),
                vmem((width, rows), bf16),
                vmem((2, 4, width, rows), bf16),
                vmem((columns // 128, 128), f32),
                vmem((1, width), f32),
                vmem((width, width), f32),
                dma((SLOTS, ROW_BLOCKS)),
                dma((SLOTS + 2,)),
                dma((2,)),
                dma((2,)),
                dma((groups, 4)),
                dma((groups, 4)),
                dma((groups, chunks)),
                dma((groups, chunks)),
                dma((groups, chunks)),
                dma((groups, chunks)),
                dma((ROW_BLOCKS, groups, 3)),
                dma((ROW_BLOCKS, groups, 3)),
                dma((2, groups, 3)),
                dma((2, groups, 3)),
                dma((SLOTS,)),
                dma((SLOTS,)),
                dma((SLOTS,)),
            ],
            compiler_params=pltpu.CompilerParams(
                collective_id=0, has_side_effects=True, vmem_limit_bytes=67_000_000),
        )(design, targets, coef_init, step_sizes.reshape(columns // 128, 128), ridge_weights.reshape(1, width))
        here = lax.axis_index("samp").astype(jnp.int32).reshape(1)
        swap = [(i, samp_size - 1 - i) for i in range(samp_size)]
        arrived = [lax.ppermute(piece, "samp", swap) for piece in pieces]
        shape = (columns, width)
        coef, resid = place(None, near, here, sum(PIECES), shape, resid)
        for half, parts in ((here, pieces), (1 - here, arrived)):
            first = 0
            for piece, n in zip(parts, PIECES):
                (coef,) = place(coef, piece, half, first, shape)
                if half is here and first == 0:
                    (coef,) = place(coef, far, 1 - here, sum(PIECES), shape)
                first += n
        return coef, resid

    return jax.shard_map(
        local_sweeps, mesh=mesh, in_specs=(design_spec, rows_spec, coef_spec, step_spec, ridge_spec),
        out_specs=(coef_spec, rows_spec), check_vma=False)
```

```python
import functools

import jax
import jax.numpy as jnp
from jax import lax
from jax.experimental import pallas as pl
from jax.experimental.pallas import tpu as pltpu
from jax.sharding import PartitionSpec as P

SWEEPS = 4
STEP_WEIGHT = 0.5
CHUNK = 1024
SLOTS = 4
GROUPS = ((0, 64), (64, 64))
SHIPPED = 512
ROW_BLOCKS = 4
KEPT = 4
PIECES = (6, 5, 1)
MESH = pl.DeviceIdType.MESH


def dot_t(left, right):
    return lax.dot_general(left, right, (((1,), (1,)), ((), ())), preferred_element_type=jnp.float32)


def sweep_kernel(
    total_rows, x_hbm, y_hbm, w0_hbm, eta_hbm, lam_hbm,
    r_hbm, shipped_hbm, w_near, w_far, *rest,
):
    w_pieces, rest = rest[: len(PIECES)], rest[len(PIECES):]
    (
        xbuf, turned, w0buf, gsend, grecv, sbuf, wt, ut, acc, rt, rbt, ra, uall, eta_ref, lam_ref, lam_col,
        x_sem, w0_sem, in_sem, ship_sem, r_send, r_recv, g_send, g_recv, s_send, s_recv, f_send, f_recv, u_send, u_recv, w_send, w_recv, out_sem,
    ) = rest
    z, s, f = lax.axis_index("problem"), lax.axis_index("samp"), lax.axis_index("feat")
    chunks, targets, _ = wt.shape
    core, chip = f % 2, f // 2
    near = chip * 2 + (1 - core)
    far = (1 - chip) * 2 + core
    partner_id = (z, 1 - s, f)
    near_id, far_id = (z, s, near), (z, s, far)
    own, other = s, 1 - s

    barrier = pltpu.get_barrier_semaphore()
    for device in (partner_id, near_id, far_id):
        pl.semaphore_signal(barrier, inc=1, device_id=device, device_id_type=MESH)

    def columns_of(chunk):
        return pl.ds(pl.multiple_of(chunk * CHUNK, CHUNK), CHUNK)

    def x_load(chunk, slot):
        return pltpu.make_async_copy(x_hbm.at[:, columns_of(chunk)], xbuf.at[slot], x_sem.at[slot, 0])

    def w0_load(chunk, slot):
        return pltpu.make_async_copy(w0_hbm.at[columns_of(chunk), :], w0buf.at[slot], w0_sem.at[slot])

    def part(ref, g, k):
        return ref.at[k, pl.ds(*GROUPS[g]), :]

    def rows_of(g):
        return pl.ds(*GROUPS[g])

    def g_copy(g, k):
        return pltpu.make_async_remote_copy(
            src_ref=part(gsend, g, k), dst_ref=part(grecv, g, k), send_sem=g_send.at[g, k], recv_sem=g_recv.at[g, k],
            device_id=partner_id, device_id_type=MESH)

    def s_copy(g, k):
        return pltpu.make_async_remote_copy(
            src_ref=part(sbuf, g, k), dst_ref=part(sbuf, g, chunks + k), send_sem=s_send.at[g, k], recv_sem=s_recv.at[g, k],
            device_id=partner_id, device_id_type=MESH)

    def u_copy(parity, g, slot, which, device):
        rows = uall.at[parity, slot, rows_of(g), :]
        return pltpu.make_async_remote_copy(
            src_ref=rows, dst_ref=rows,
            send_sem=u_send.at[parity, g, which], recv_sem=u_recv.at[parity, g, which],
            device_id=device, device_id_type=MESH)

    ahead = SLOTS - 1

    def start(copy):
        copy.start(priority=1)

    def wait(copy):
        copy.wait()

    def other_load(i, slot, act):
        act(x_load(other * chunks + i, slot))

    def own_load(i, slot, act):
        @pl.when(i != chunks - 1)
        def _():
            act(x_load(own * chunks + i - i // chunks, slot))

        @pl.when(i == chunks - 1)
        def _():
            act(pltpu.make_async_copy(shipped_hbm, xbuf.at[slot, :, pl.ds(0, SHIPPED)], x_sem.at[slot, 0]))

    def steps(base, count, load, next_load, body, more=None):
        def step(i, carry):
            upcoming = i + ahead
            slot = (base + upcoming) % SLOTS

            @pl.when(upcoming < count)
            def _():
                load(upcoming, slot, start)

            wanted = upcoming >= count
            if more is not None:
                wanted = jnp.logical_and(wanted, more)

            @pl.when(wanted)
            def _():
                next_load(upcoming - count, slot, start)

            load(i, (base + i) % SLOTS, wait)
            body(i, (base + i) % SLOTS)
            return carry

        lax.fori_loop(0, count, step, 0)

    rows = x_hbm.shape[0] // ROW_BLOCKS
    width = xbuf.shape[1] // rows
    passes = 2 * chunks // width
    blocks = ROW_BLOCKS * passes
    pairs = w0buf.shape[0] // 2

    def tile_load(step, q):
        slot = step % SLOTS
        where = pl.ds(pl.multiple_of(step // passes * rows, rows), rows)
        return pltpu.make_async_copy(
            x_hbm.at[where, columns_of(step % passes * width + q)], xbuf.at[slot, pl.ds(q * rows, rows), :], x_sem.at[slot, q])

    def tiles_ahead(step):
        upcoming = step + ahead

        @pl.when(upcoming < blocks)
        def _():
            for q in range(width):
                tile_load(upcoming, q).start(priority=1)

        @pl.when(upcoming >= blocks)
        def _():
            x_load(other * chunks + upcoming - blocks, upcoming % SLOTS).start(priority=1)

    def w0_pair(pair, q):
        return w0_load(2 * pair + q, 2 * (pair % pairs) + q)

    eta_load = pltpu.make_async_copy(eta_hbm, eta_ref, in_sem.at[0])
    lam_load = pltpu.make_async_copy(lam_hbm, lam_ref, in_sem.at[1])
    halves = [
        pltpu.make_async_copy(
            y_hbm.at[pl.ds(i * CHUNK, CHUNK), :], w0buf.at[2 * pairs - 2 + i], w0_sem.at[2 * pairs - 2 + i])
        for i in range(2)
    ]
    for load in (*halves, lam_load, eta_load):
        load.start()
    for pair in range(pairs - 1):
        for q in range(2):
            w0_pair(pair, q).start()
    for step in range(ahead):
        for q in range(width):
            tile_load(step, q).start(priority=1)
    ut[...] = jnp.zeros_like(ut)
    acc[...] = jnp.zeros_like(acc)
    for i, load in enumerate(halves):
        load.wait()
        rt[:, i * CHUNK:(i + 1) * CHUNK] = w0buf[2 * pairs - 2 + i].T
    pl.semaphore_wait(barrier, 3)
    ship = pltpu.make_async_remote_copy(
        src_ref=x_hbm.at[:, pl.ds(pl.multiple_of((other + 1) * chunks * CHUNK - SHIPPED, 128), SHIPPED)],
        dst_ref=shipped_hbm, send_sem=ship_sem.at[0], recv_sem=ship_sem.at[1],
        device_id=partner_id, device_id_type=MESH)
    ship.start()
    lam_load.wait()
    lam_col[...] = jnp.broadcast_to(lam_ref[0:1, :], (targets, targets)).T

    def first_pass(pair, carry):
        @pl.when(pair % (width // 2) == 0)
        def _():
            tiles_ahead(pair // (width // 2))

        @pl.when(pair + pairs - 1 < chunks)
        def _():
            for q in range(2):
                w0_pair(pair + pairs - 1, q).start()

        slot = pair // (width // 2) % SLOTS
        first = pair % (width // 2) * 2
        total = acc[...]
        for q in range(2):
            w0_pair(pair, q).wait()
            tile_load(pair // (width // 2), first + q).wait()
        for q in range(2):
            weights = w0buf[2 * (pair % pairs) + q].T.astype(jnp.bfloat16)
            sbuf[2 * pair + q] = weights
            where = pl.ds(pl.multiple_of((first + q) * rows, rows), rows)
            total += dot_t(weights, xbuf[slot, where, :])
        acc[...] = total
        return carry

    def block_product(weights, tiles):
        plain = len(tiles) // 2
        for q, tile in enumerate(tiles[plain:]):
            turned[q] = tile.T
        total = sum(dot_t(weight, tile) for weight, tile in zip(weights[:plain], tiles))
        for q, weight in enumerate(weights[plain:]):
            total += jnp.dot(weight, turned[q], preferred_element_type=jnp.float32)
        return total

    def later_pass(block, carry):
        def step_(i, inner):
            step = block * passes + i
            tiles_ahead(step)
            for q in range(width):
                tile_load(step, q).wait()
            slot = step % SLOTS
            acc[...] += block_product(
                [sbuf[i * width + q] for q in range(width)],
                [xbuf[slot, q * rows:(q + 1) * rows, :] for q in range(width)])
            return inner

        lax.fori_loop(0, passes, step_, 0)
        return carry

    def lanes_of(block):
        return pl.ds(block * rows, rows)

    def first_copy(block, g, slot, which, device):
        ref = uall.at[0, slot, rows_of(g), lanes_of(block)]
        return pltpu.make_async_remote_copy(
            src_ref=ref, dst_ref=ref, send_sem=f_send.at[block, g, which], recv_sem=f_recv.at[block, g, which],
            device_id=device, device_id_type=MESH)

    def first_begin(block):
        uall[0, f, :, lanes_of(block)] = acc[...].astype(jnp.bfloat16)
        acc[...] = jnp.zeros_like(acc)
        for g in range(len(GROUPS)):
            first_copy(block, g, f, 0, near_id).start()
            first_copy(block, g, f, 1, far_id).start()

    def first_forward(block, g):
        first_copy(block, g, far, 1, far_id).wait_recv()
        first_copy(block, g, far, 2, near_id).start()

    def first_end(block, g):
        first_copy(block, g, near, 0, near_id).wait_recv()
        first_copy(block, g, far, 2, near_id).wait_recv()
        total = uall[0, 0, rows_of(g), lanes_of(block)].astype(jnp.float32)
        for j in range(1, 4):
            total += uall[0, j, rows_of(g), lanes_of(block)].astype(jnp.float32)
        new = rt[rows_of(g), lanes_of(block)] - total
        rt[rows_of(g), lanes_of(block)] = new
        rbt[rows_of(g), lanes_of(block)] = new.astype(jnp.bfloat16)
        first_copy(block, g, f, 0, near_id).wait_send()
        first_copy(block, g, f, 1, far_id).wait_send()
        first_copy(block, g, far, 2, near_id).wait_send()

    lax.fori_loop(0, chunks, first_pass, 0)
    last = ROW_BLOCKS - 1
    for block in range(ROW_BLOCKS):
        if block:
            later_pass(block, 0)
        first_begin(block)
        for g in range(len(GROUPS)):
            if block >= 1:
                first_forward(block - 1, g)
            if block >= 2:
                first_end(block - 2, g)

    def u_begin(parity, g):
        uall[parity, f, rows_of(g), :] = ut[rows_of(g), :].astype(jnp.bfloat16)
        ut[rows_of(g), :] = jnp.zeros((GROUPS[g][1], ut.shape[1]), jnp.float32)
        u_copy(parity, g, f, 0, near_id).start()
        u_copy(parity, g, f, 1, far_id).start()

    def u_end(parity, g):
        u_copy(parity, g, far, 1, far_id).wait_recv()
        u_copy(parity, g, far, 2, near_id).start()
        u_copy(parity, g, near, 0, near_id).wait_recv()
        u_copy(parity, g, far, 2, near_id).wait_recv()
        total = uall[parity, 0, rows_of(g), :].astype(jnp.float32)
        for block in range(1, 4):
            total += uall[parity, block, rows_of(g), :].astype(jnp.float32)
        new = rt[rows_of(g), :] - STEP_WEIGHT * total
        rt[rows_of(g), :] = new
        rbt[rows_of(g), :] = new.astype(jnp.bfloat16)
        u_copy(parity, g, f, 0, near_id).wait_send()
        u_copy(parity, g, f, 1, far_id).wait_send()
        u_copy(parity, g, far, 2, near_id).wait_send()

    quarter = ra.shape[1] // 4

    def r_copy(g, source, of, which, device):
        lanes = pl.ds(pl.multiple_of(of * quarter, quarter), quarter)
        return pltpu.make_async_remote_copy(
            src_ref=source.at[rows_of(g), lanes], dst_ref=ra.at[rows_of(g), lanes],
            send_sem=r_send.at[g, which], recv_sem=r_recv.at[g, which], device_id=device, device_id_type=MESH)

    def r_begin(g):
        r_copy(g, rbt, f, 0, partner_id).start()

    def r_spread(g):
        r_copy(g, rbt, f, 0, partner_id).wait()
        r_copy(g, ra, f, 1, near_id).start()
        r_copy(g, ra, f, 2, far_id).start()

    def r_end(g):
        r_copy(g, ra, far, 2, far_id).wait_recv()
        r_copy(g, ra, far, 3, near_id).start()
        r_copy(g, ra, near, 1, near_id).wait_recv()
        r_copy(g, ra, far, 3, near_id).wait_recv()
        r_copy(g, ra, f, 1, near_id).wait_send()
        r_copy(g, ra, f, 2, far_id).wait_send()
        r_copy(g, ra, far, 3, near_id).wait_send()

    sent = CHUNK - SHIPPED

    def last_copy(g):
        lanes = pl.ds(0, sent)
        return pltpu.make_async_remote_copy(
            src_ref=gsend.at[chunks - 1, rows_of(g), lanes], dst_ref=grecv.at[chunks - 1, rows_of(g), lanes],
            send_sem=g_send.at[g, chunks - 1], recv_sem=g_recv.at[g, chunks - 1],
            device_id=partner_id, device_id_type=MESH)

    def for_g_copy(g, k, act):
        @pl.when(k < chunks - 1)
        def _():
            act(g_copy(g, k))

        @pl.when(k == chunks - 1)
        def _():
            act(last_copy(g))

    def partner_gradient(g, base, next_load):
        def body(k, slot):
            gsend[k, rows_of(g), :] = jnp.dot(rbt[rows_of(g), :], xbuf[slot], preferred_element_type=jnp.float32)
            for_g_copy(g, k, lambda copy: copy.start())

        steps(base, chunks, other_load, next_load, body)

    def own_columns(g, t, base, next_load):
        lam = lam_col[rows_of(g), 0:1]

        def body(i, slot):
            @pl.when(i == chunks - 1)
            def _():
                r_end(g)
                grecv[chunks - 1, rows_of(g), sent:] = jnp.dot(
                    ra[rows_of(g), :], xbuf[slot, :, 0:SHIPPED], preferred_element_type=jnp.float32)

            @pl.when(i != chunks - 1)
            def _():
                k = i - i // chunks
                for_g_copy(g, k, lambda copy: copy.wait_recv())

                @pl.when(t > 0)
                def _():
                    s_copy(g, k).wait_send()

                mine = jnp.dot(rbt[rows_of(g), :], xbuf[slot], preferred_element_type=jnp.float32)
                weights = wt[k, rows_of(g), :]
                gradient = (mine + grecv[k, rows_of(g), :]) * (1.0 / total_rows)
                lanes = eta_ref.shape[1]
                first = (own * chunks + k) * (CHUNK // lanes)
                eta = jnp.concatenate([eta_ref[pl.ds(first + j, 1), :] for j in range(CHUNK // lanes)], axis=1)
                delta = eta * (gradient - lam * weights)
                wt[k, rows_of(g), :] = weights + STEP_WEIGHT * delta
                delta_b = delta.astype(jnp.bfloat16)
                sbuf[k, rows_of(g), :] = delta_b
                ut[rows_of(g), :] += dot_t(delta_b, xbuf[slot])
                s_copy(g, k).start()

        steps(base, chunks + 1, own_load, next_load, body)

    def partner_columns(g, base, next_load, more=None):
        def body(k, slot):
            s_copy(g, k).wait_recv()
            for_g_copy(g, k, lambda copy: copy.wait_send())
            ut[rows_of(g), :] += dot_t(sbuf[chunks + k, rows_of(g), :], xbuf[slot])

        steps(base, chunks, other_load, next_load, body, more)

    first_forward(last, 0)
    first_end(last - 1, 0)
    first_end(last, 0)
    r_begin(0)
    first_forward(last, 1)
    partner_gradient(0, blocks, other_load)
    first_end(last - 1, 1)
    first_end(last, 1)
    r_begin(1)
    partner_gradient(1, blocks, own_load)

    eta_load.wait()
    for k in range(ahead):
        w0_load(own * chunks + k, k).start()

    def keep(k, carry):
        @pl.when(k + ahead < chunks)
        def _():
            w0_load(own * chunks + k + ahead, (k + ahead) % SLOTS).start()

        w0_load(own * chunks + k, k % SLOTS).wait()
        wt[k] = w0buf[k % SLOTS].T
        return carry

    lax.fori_loop(0, chunks, keep, 0)
    ship.wait()
    r_spread(0)

    def w_store(ref, first, n, k):
        rows = pl.ds(pl.multiple_of(k * CHUNK, CHUNK), CHUNK)
        slot = (first + k) % SLOTS
        return pltpu.make_async_copy(w0buf.at[slot], ref.at[rows, :], out_sem.at[slot])

    def w_copy(k):
        rows = pl.ds(pl.multiple_of(k * CHUNK, CHUNK), CHUNK)
        slot = k % SLOTS
        return pltpu.make_async_remote_copy(
            src_ref=w0buf.at[slot], dst_ref=w_far.at[rows, :], send_sem=w_send.at[slot], recv_sem=w_recv.at[slot],
            device_id=partner_id, device_id_type=MESH)

    def w_out():
        first = 0
        for ref, n in (*zip(w_pieces, PIECES), (w_near, KEPT)):

            def put(k, carry, ref=ref, n=n, first=first):
                chunk = first + k
                slot = chunk % SLOTS

                @pl.when(chunk >= SLOTS)
                def _():
                    w_store(ref, first, n, k).wait()

                w0buf[slot] = wt[chunk].T
                w_store(ref, first, n, k).start()
                return carry

            lax.fori_loop(0, n, put, 0)
            first += n

        def send(k, carry):
            w_copy(k).start()
            return carry

        lax.fori_loop(0, KEPT, send, 0)

    def sweep(t, carry):
        parity = (t + 1) % 2
        more = t < SWEEPS - 1
        at = t * (6 * chunks + 2)
        own_columns(0, t, at, own_load)
        r_spread(1)
        own_columns(1, t, at + chunks + 1, other_load)

        @pl.when(jnp.logical_not(more))
        def _():
            w_out()

        at = at + 2 * chunks + 2
        partner_columns(0, at, other_load)
        u_begin(parity, 0)
        u_end(parity, 0)

        @pl.when(more)
        def _():
            r_begin(0)
            partner_gradient(0, at, other_load)

        partner_columns(1, at, other_load, more)

        @pl.when(more)
        def _():
            r_spread(0)

        u_begin(parity, 1)
        u_end(parity, 1)

        @pl.when(more)
        def _():
            r_begin(1)
            partner_gradient(1, at, own_load)

        return carry

    lax.fori_loop(0, SWEEPS, sweep, 0)
    r_stores = []
    for i in range(2):
        w0buf[SLOTS + i] = rt[:, i * CHUNK:(i + 1) * CHUNK].T
        r_stores.append(
            pltpu.make_async_copy(w0buf.at[SLOTS + i], r_hbm.at[pl.ds(i * CHUNK, CHUNK), :], in_sem.at[i]))
        r_stores[i].start()

    def drain(k, carry):
        for g in range(len(GROUPS)):
            s_copy(g, k).wait_send()
        return carry

    lax.fori_loop(0, chunks, drain, 0)
    for k in range(KEPT):
        w_store(w_near, sum(PIECES), KEPT, k).wait()
        w_copy(k).wait()
    for store in r_stores:
        store.wait()


def place(result, piece, half, first, shape, extra=None):
    rows, width = piece.shape
    halves = shape[0] // CHUNK // 2
    here = pl.BlockSpec((CHUNK, width), lambda i, half_ref: (half_ref[0] * halves + first + i, 0))
    out_shape, out_specs = [jax.ShapeDtypeStruct(shape, piece.dtype)], [here]

    def body(half_ref, piece_ref, other_ref, out_ref, *copied):
        out_ref[...] = piece_ref[...]
        for ref in copied:
            ref[...] = other_ref[...]

    if result is None:
        whole = pl.BlockSpec(extra.shape, lambda i, half_ref: (0, 0))
        out_shape.append(jax.ShapeDtypeStruct(extra.shape, extra.dtype))
        out_specs.append(whole)
        other, other_spec, aliases = extra, whole, {}
    else:
        other, other_spec, aliases = result, pl.BlockSpec(memory_space=pl.ANY), {2: 0}
    return pl.pallas_call(
        body,
        name="place",
        out_shape=out_shape,
        grid_spec=pltpu.PrefetchScalarGridSpec(
            num_scalar_prefetch=1,
            grid=(rows // CHUNK,),
            in_specs=[pl.BlockSpec((CHUNK, width), lambda i, half_ref: (i, 0)), other_spec],
            out_specs=out_specs,
        ),
        input_output_aliases=aliases,
    )(half, piece, other)


def solution(mesh):
    samp_size = mesh.shape["samp"]
    design_spec = P(("problem", "samp"), "feat")
    rows_spec = P(("problem", "samp"), None)
    coef_spec = P(("problem", "feat"), None)
    step_spec = P(("problem", "feat"))
    ridge_spec = P("problem")

    def local_sweeps(design, targets, coef_init, step_sizes, ridge_weights):
        rows, columns = design.shape
        width = targets.shape[1]
        groups = len(GROUPS)
        chunks = columns // CHUNK // samp_size
        bf16, f32 = jnp.bfloat16, jnp.float32
        vmem, dma = pltpu.VMEM, pltpu.SemaphoreType.DMA
        in_hbm = pl.BlockSpec(memory_space=pltpu.HBM)
        sizes = (KEPT, KEPT, *PIECES)
        resid, _, near, far, *pieces = pl.pallas_call(
            functools.partial(sweep_kernel, rows * samp_size),
            name="sweeps",
            out_shape=(
                jax.ShapeDtypeStruct((rows, width), f32),
                jax.ShapeDtypeStruct((rows, SHIPPED), bf16),
                *(jax.ShapeDtypeStruct((n * CHUNK, width), f32) for n in sizes),
            ),
            in_specs=[in_hbm] * 5,
            out_specs=(in_hbm,) * (2 + len(sizes)),
            scratch_shapes=[
                vmem((SLOTS, rows, CHUNK), bf16),
                vmem((2, CHUNK, rows // ROW_BLOCKS), bf16),
                vmem((SLOTS + 2, CHUNK, width), f32),
                vmem((chunks, width, CHUNK), f32),
                vmem((chunks, width, CHUNK), f32),
                vmem((2 * chunks, width, CHUNK), bf16),
                vmem((chunks, width, CHUNK), f32),
                vmem((width, rows), f32),
                vmem((width, rows // ROW_BLOCKS), f32),
                vmem((width, rows), f32),
                vmem((width, rows), bf16),
                vmem((width, rows), bf16),
                vmem((2, 4, width, rows), bf16),
                vmem((columns // 128, 128), f32),
                vmem((1, width), f32),
                vmem((width, width), f32),
                dma((SLOTS, ROW_BLOCKS)),
                dma((SLOTS + 2,)),
                dma((2,)),
                dma((2,)),
                dma((groups, 4)),
                dma((groups, 4)),
                dma((groups, chunks)),
                dma((groups, chunks)),
                dma((groups, chunks)),
                dma((groups, chunks)),
                dma((ROW_BLOCKS, groups, 3)),
                dma((ROW_BLOCKS, groups, 3)),
                dma((2, groups, 3)),
                dma((2, groups, 3)),
                dma((SLOTS,)),
                dma((SLOTS,)),
                dma((SLOTS,)),
            ],
            compiler_params=pltpu.CompilerParams(
                collective_id=0, has_side_effects=True, vmem_limit_bytes=67_000_000),
        )(design, targets, coef_init, step_sizes.reshape(columns // 128, 128), ridge_weights.reshape(1, width))
        here = lax.axis_index("samp").astype(jnp.int32).reshape(1)
        swap = [(i, samp_size - 1 - i) for i in range(samp_size)]
        arrived = [lax.ppermute(piece, "samp", swap) for piece in pieces]
        shape = (columns, width)
        coef, resid = place(None, near, here, sum(PIECES), shape, resid)
        for half, parts in ((here, pieces), (1 - here, arrived)):
            first = 0
            for piece, n in zip(parts, PIECES):
                (coef,) = place(coef, piece, half, first, shape)
                if half is here and first == 0:
                    (coef,) = place(coef, far, 1 - here, sum(PIECES), shape)
                first += n
        return coef, resid

    return jax.shard_map(
        local_sweeps, mesh=mesh, in_specs=(design_spec, rows_spec, coef_spec, step_spec, ridge_spec),
        out_specs=(coef_spec, rows_spec), check_vma=False)
```

```python
import functools

import jax
import jax.numpy as jnp
from jax import lax
from jax.experimental import pallas as pl
from jax.experimental.pallas import tpu as pltpu
from jax.sharding import PartitionSpec as P

SWEEPS = 4
STEP_WEIGHT = 0.5
CHUNK = 1024
SLOTS = 4
GROUPS = ((0, 48), (48, 80))
SHIPPED = 512
EXTRA = 128
ROW_BLOCKS = 4
KEPT = 4
PIECES = (6, 5, 1)
MESH = pl.DeviceIdType.MESH


def dot_t(left, right):
    return lax.dot_general(left, right, (((1,), (1,)), ((), ())), preferred_element_type=jnp.float32)


def sweep_kernel(
    total_rows, x_hbm, y_hbm, w0_hbm, eta_hbm, lam_hbm,
    r_hbm, shipped_hbm, w_near, w_far, *rest,
):
    w_pieces, rest = rest[: len(PIECES)], rest[len(PIECES):]
    (
        xbuf, turned, w0buf, gsend, grecv, sbuf, wt, ut, acc, rt, rbt, ra, uall, eta_ref, lam_ref, lam_col,
        x_sem, w0_sem, in_sem, ship_sem, r_send, r_recv, g_send, g_recv, s_send, s_recv, f_send, f_recv, u_send, u_recv, w_send, w_recv, out_sem,
    ) = rest
    z, s, f = lax.axis_index("problem"), lax.axis_index("samp"), lax.axis_index("feat")
    chunks, targets, _ = wt.shape
    core, chip = f % 2, f // 2
    near = chip * 2 + (1 - core)
    far = (1 - chip) * 2 + core
    partner_id = (z, 1 - s, f)
    near_id, far_id = (z, s, near), (z, s, far)
    own, other = s, 1 - s

    barrier = pltpu.get_barrier_semaphore()
    for device in (partner_id, near_id, far_id):
        pl.semaphore_signal(barrier, inc=1, device_id=device, device_id_type=MESH)

    def columns_of(chunk):
        return pl.ds(pl.multiple_of(chunk * CHUNK, CHUNK), CHUNK)

    def x_load(chunk, slot):
        return pltpu.make_async_copy(x_hbm.at[:, columns_of(chunk)], xbuf.at[slot], x_sem.at[slot, 0])

    def w0_load(chunk, slot):
        return pltpu.make_async_copy(w0_hbm.at[columns_of(chunk), :], w0buf.at[slot], w0_sem.at[slot])

    def part(ref, g, k):
        return ref.at[k, pl.ds(*GROUPS[g]), :]

    def rows_of(g):
        return pl.ds(*GROUPS[g])

    def g_copy(g, k):
        return pltpu.make_async_remote_copy(
            src_ref=part(gsend, g, k), dst_ref=part(grecv, g, k), send_sem=g_send.at[g, k], recv_sem=g_recv.at[g, k],
            device_id=partner_id, device_id_type=MESH)

    def s_copy(g, k):
        return pltpu.make_async_remote_copy(
            src_ref=part(sbuf, g, k), dst_ref=part(sbuf, g, chunks + k), send_sem=s_send.at[g, k], recv_sem=s_recv.at[g, k],
            device_id=partner_id, device_id_type=MESH)

    def u_copy(parity, g, slot, which, device):
        rows = uall.at[parity, slot, rows_of(g), :]
        return pltpu.make_async_remote_copy(
            src_ref=rows, dst_ref=rows,
            send_sem=u_send.at[parity, g, which], recv_sem=u_recv.at[parity, g, which],
            device_id=device, device_id_type=MESH)

    ahead = SLOTS - 1

    def start(copy):
        copy.start(priority=1)

    def wait(copy):
        copy.wait()

    def other_load(i, slot, act):
        act(x_load(other * chunks + i, slot))

    def for_ship(act):
        @pl.when(core == 0)
        def _():
            act(pl.ds(0, EXTRA + SHIPPED))

        @pl.when(core == 1)
        def _():
            act(pl.ds(EXTRA, SHIPPED))

    def own_load(i, slot, act):
        @pl.when(i != chunks - 1)
        def _():
            act(x_load(own * chunks + i - i // chunks, slot))

        @pl.when(i == chunks - 1)
        def _():
            for_ship(
                lambda where: act(
                    pltpu.make_async_copy(shipped_hbm.at[:, where], xbuf.at[slot, :, where], x_sem.at[slot, 0])))

    def steps(base, count, load, next_load, body, more=None):
        def step(i, carry):
            upcoming = i + ahead
            slot = (base + upcoming) % SLOTS

            @pl.when(upcoming < count)
            def _():
                load(upcoming, slot, start)

            wanted = upcoming >= count
            if more is not None:
                wanted = jnp.logical_and(wanted, more)

            @pl.when(wanted)
            def _():
                next_load(upcoming - count, slot, start)

            load(i, (base + i) % SLOTS, wait)
            body(i, (base + i) % SLOTS)
            return carry

        lax.fori_loop(0, count, step, 0)

    rows = x_hbm.shape[0] // ROW_BLOCKS
    width = xbuf.shape[1] // rows
    passes = 2 * chunks // width
    blocks = ROW_BLOCKS * passes
    pairs = w0buf.shape[0] // 2

    def tile_load(step, q):
        slot = step % SLOTS
        where = pl.ds(pl.multiple_of(step // passes * rows, rows), rows)
        return pltpu.make_async_copy(
            x_hbm.at[where, columns_of(step % passes * width + q)], xbuf.at[slot, pl.ds(q * rows, rows), :], x_sem.at[slot, q])

    def tiles_ahead(step):
        upcoming = step + ahead

        @pl.when(upcoming < blocks)
        def _():
            for q in range(width):
                tile_load(upcoming, q).start(priority=1)

        @pl.when(upcoming >= blocks)
        def _():
            x_load(other * chunks + upcoming - blocks, upcoming % SLOTS).start(priority=1)

    def w0_pair(pair, q):
        return w0_load(2 * pair + q, 2 * (pair % pairs) + q)

    eta_load = pltpu.make_async_copy(eta_hbm, eta_ref, in_sem.at[0])
    lam_load = pltpu.make_async_copy(lam_hbm, lam_ref, in_sem.at[1])
    halves = [
        pltpu.make_async_copy(
            y_hbm.at[pl.ds(i * CHUNK, CHUNK), :], w0buf.at[2 * pairs - 2 + i], w0_sem.at[2 * pairs - 2 + i])
        for i in range(2)
    ]
    for load in (*halves, lam_load, eta_load):
        load.start()
    for pair in range(pairs - 1):
        for q in range(2):
            w0_pair(pair, q).start()
    for step in range(ahead):
        for q in range(width):
            tile_load(step, q).start(priority=1)
    ut[...] = jnp.zeros_like(ut)
    acc[...] = jnp.zeros_like(acc)
    for i, load in enumerate(halves):
        load.wait()
        rt[:, i * CHUNK:(i + 1) * CHUNK] = w0buf[2 * pairs - 2 + i].T
    pl.semaphore_wait(barrier, 3)

    def ship(where):
        first = (other + 1) * chunks * CHUNK - EXTRA - SHIPPED + where.start
        return pltpu.make_async_remote_copy(
            src_ref=x_hbm.at[:, pl.ds(pl.multiple_of(first, 128), where.size)], dst_ref=shipped_hbm.at[:, where],
            send_sem=ship_sem.at[0], recv_sem=ship_sem.at[1], device_id=partner_id, device_id_type=MESH)

    for_ship(lambda where: ship(where).start())
    lam_load.wait()
    lam_col[...] = jnp.broadcast_to(lam_ref[0:1, :], (targets, targets)).T

    def first_pass(pair, carry):
        @pl.when(pair % (width // 2) == 0)
        def _():
            tiles_ahead(pair // (width // 2))

        @pl.when(pair + pairs - 1 < chunks)
        def _():
            for q in range(2):
                w0_pair(pair + pairs - 1, q).start()

        slot = pair // (width // 2) % SLOTS
        first = pair % (width // 2) * 2
        total = acc[...]
        for q in range(2):
            w0_pair(pair, q).wait()
            tile_load(pair // (width // 2), first + q).wait()
        for q in range(2):
            weights = w0buf[2 * (pair % pairs) + q].T.astype(jnp.bfloat16)
            sbuf[2 * pair + q] = weights
            where = pl.ds(pl.multiple_of((first + q) * rows, rows), rows)
            total += dot_t(weights, xbuf[slot, where, :])
        acc[...] = total
        return carry

    def block_product(weights, tiles):
        plain = len(tiles) // 2
        for q, tile in enumerate(tiles[plain:]):
            turned[q] = tile.T
        total = sum(dot_t(weight, tile) for weight, tile in zip(weights[:plain], tiles))
        for q, weight in enumerate(weights[plain:]):
            total += jnp.dot(weight, turned[q], preferred_element_type=jnp.float32)
        return total

    def later_pass(block, carry):
        def step_(i, inner):
            step = block * passes + i
            tiles_ahead(step)
            for q in range(width):
                tile_load(step, q).wait()
            slot = step % SLOTS
            acc[...] += block_product(
                [sbuf[i * width + q] for q in range(width)],
                [xbuf[slot, q * rows:(q + 1) * rows, :] for q in range(width)])
            return inner

        lax.fori_loop(0, passes, step_, 0)
        return carry

    def lanes_of(block):
        return pl.ds(block * rows, rows)

    def first_copy(block, g, slot, which, device):
        ref = uall.at[0, slot, rows_of(g), lanes_of(block)]
        return pltpu.make_async_remote_copy(
            src_ref=ref, dst_ref=ref, send_sem=f_send.at[block, g, which], recv_sem=f_recv.at[block, g, which],
            device_id=device, device_id_type=MESH)

    def first_begin(block):
        uall[0, f, :, lanes_of(block)] = acc[...].astype(jnp.bfloat16)
        acc[...] = jnp.zeros_like(acc)
        for g in range(len(GROUPS)):
            first_copy(block, g, f, 0, near_id).start()
            first_copy(block, g, f, 1, far_id).start()

    def first_forward(block, g):
        first_copy(block, g, far, 1, far_id).wait_recv()
        first_copy(block, g, far, 2, near_id).start()

    def first_end(block, g):
        first_copy(block, g, near, 0, near_id).wait_recv()
        first_copy(block, g, far, 2, near_id).wait_recv()
        total = uall[0, 0, rows_of(g), lanes_of(block)].astype(jnp.float32)
        for j in range(1, 4):
            total += uall[0, j, rows_of(g), lanes_of(block)].astype(jnp.float32)
        new = rt[rows_of(g), lanes_of(block)] - total
        rt[rows_of(g), lanes_of(block)] = new
        rbt[rows_of(g), lanes_of(block)] = new.astype(jnp.bfloat16)
        first_copy(block, g, f, 0, near_id).wait_send()
        first_copy(block, g, f, 1, far_id).wait_send()
        first_copy(block, g, far, 2, near_id).wait_send()

    lax.fori_loop(0, chunks, first_pass, 0)
    last = ROW_BLOCKS - 1
    for block in range(ROW_BLOCKS):
        if block:
            later_pass(block, 0)
        first_begin(block)
        for g in range(len(GROUPS)):
            if block >= 1:
                first_forward(block - 1, g)
            if block >= 2:
                first_end(block - 2, g)

    def u_begin(parity, g):
        uall[parity, f, rows_of(g), :] = ut[rows_of(g), :].astype(jnp.bfloat16)
        ut[rows_of(g), :] = jnp.zeros((GROUPS[g][1], ut.shape[1]), jnp.float32)
        u_copy(parity, g, f, 0, near_id).start()
        u_copy(parity, g, f, 1, far_id).start()

    def u_end(parity, g):
        u_copy(parity, g, far, 1, far_id).wait_recv()
        u_copy(parity, g, far, 2, near_id).start()
        u_copy(parity, g, near, 0, near_id).wait_recv()
        u_copy(parity, g, far, 2, near_id).wait_recv()
        total = uall[parity, 0, rows_of(g), :].astype(jnp.float32)
        for block in range(1, 4):
            total += uall[parity, block, rows_of(g), :].astype(jnp.float32)
        new = rt[rows_of(g), :] - STEP_WEIGHT * total
        rt[rows_of(g), :] = new
        rbt[rows_of(g), :] = new.astype(jnp.bfloat16)
        u_copy(parity, g, f, 0, near_id).wait_send()
        u_copy(parity, g, f, 1, far_id).wait_send()
        u_copy(parity, g, far, 2, near_id).wait_send()

    quarter = ra.shape[1] // 4

    def r_copy(g, source, of, which, device):
        lanes = pl.ds(pl.multiple_of(of * quarter, quarter), quarter)
        return pltpu.make_async_remote_copy(
            src_ref=source.at[rows_of(g), lanes], dst_ref=ra.at[rows_of(g), lanes],
            send_sem=r_send.at[g, which], recv_sem=r_recv.at[g, which], device_id=device, device_id_type=MESH)

    def r_begin(g):
        r_copy(g, rbt, f, 0, partner_id).start()

    def r_spread(g):
        r_copy(g, rbt, f, 0, partner_id).wait()
        r_copy(g, ra, f, 1, near_id).start()
        r_copy(g, ra, f, 2, far_id).start()

    def r_end(g):
        r_copy(g, ra, far, 2, far_id).wait_recv()
        r_copy(g, ra, far, 3, near_id).start()
        r_copy(g, ra, near, 1, near_id).wait_recv()
        r_copy(g, ra, far, 3, near_id).wait_recv()
        r_copy(g, ra, f, 1, near_id).wait_send()
        r_copy(g, ra, f, 2, far_id).wait_send()
        r_copy(g, ra, far, 3, near_id).wait_send()

    sent = CHUNK - SHIPPED

    def last_copy(g, size):
        lanes = pl.ds(0, size)
        return pltpu.make_async_remote_copy(
            src_ref=gsend.at[chunks - 1, rows_of(g), lanes], dst_ref=grecv.at[chunks - 1, rows_of(g), lanes],
            send_sem=g_send.at[g, chunks - 1], recv_sem=g_recv.at[g, chunks - 1],
            device_id=partner_id, device_id_type=MESH)

    def for_g_copy(g, k, act):
        @pl.when(k < chunks - 1)
        def _():
            act(g_copy(g, k))

        for which, size in enumerate((sent - EXTRA, sent)):

            @pl.when(jnp.logical_and(k == chunks - 1, core == which))
            def _(size=size):
                act(last_copy(g, size))

    def partner_gradient(g, base, next_load):
        def body(k, slot):
            gsend[k, rows_of(g), :] = jnp.dot(rbt[rows_of(g), :], xbuf[slot], preferred_element_type=jnp.float32)
            for_g_copy(g, k, lambda copy: copy.start())

        steps(base, chunks, other_load, next_load, body)

    def own_columns(g, t, base, next_load):
        lam = lam_col[rows_of(g), 0:1]

        def body(i, slot):
            @pl.when(i == chunks - 1)
            def _():
                r_end(g)
                grecv[chunks - 1, rows_of(g), sent:] = jnp.dot(
                    ra[rows_of(g), :], xbuf[slot, :, EXTRA:EXTRA + SHIPPED], preferred_element_type=jnp.float32)

                @pl.when(core == 0)
                def _():
                    grecv[chunks - 1, rows_of(g), sent - EXTRA:sent] = jnp.dot(
                        ra[rows_of(g), :], xbuf[slot, :, 0:EXTRA], preferred_element_type=jnp.float32)

            @pl.when(i != chunks - 1)
            def _():
                k = i - i // chunks
                for_g_copy(g, k, lambda copy: copy.wait_recv())

                @pl.when(t > 0)
                def _():
                    s_copy(g, k).wait_send()

                mine = jnp.dot(rbt[rows_of(g), :], xbuf[slot], preferred_element_type=jnp.float32)
                weights = wt[k, rows_of(g), :]
                gradient = (mine + grecv[k, rows_of(g), :]) * (1.0 / total_rows)
                lanes = eta_ref.shape[1]
                first = (own * chunks + k) * (CHUNK // lanes)
                eta = jnp.concatenate([eta_ref[pl.ds(first + j, 1), :] for j in range(CHUNK // lanes)], axis=1)
                delta = eta * (gradient - lam * weights)
                wt[k, rows_of(g), :] = weights + STEP_WEIGHT * delta
                delta_b = delta.astype(jnp.bfloat16)
                sbuf[k, rows_of(g), :] = delta_b
                ut[rows_of(g), :] += dot_t(delta_b, xbuf[slot])
                s_copy(g, k).start()

        steps(base, chunks + 1, own_load, next_load, body)

    def partner_columns(g, base, next_load, more=None):
        def body(k, slot):
            s_copy(g, k).wait_recv()
            for_g_copy(g, k, lambda copy: copy.wait_send())
            ut[rows_of(g), :] += dot_t(sbuf[chunks + k, rows_of(g), :], xbuf[slot])

        steps(base, chunks, other_load, next_load, body, more)

    first_forward(last, 0)
    first_end(last - 1, 0)
    first_end(last, 0)
    r_begin(0)
    first_forward(last, 1)
    partner_gradient(0, blocks, other_load)
    first_end(last - 1, 1)
    first_end(last, 1)
    r_begin(1)
    partner_gradient(1, blocks, own_load)

    eta_load.wait()
    for k in range(ahead):
        w0_load(own * chunks + k, k).start()

    def keep(k, carry):
        @pl.when(k + ahead < chunks)
        def _():
            w0_load(own * chunks + k + ahead, (k + ahead) % SLOTS).start()

        w0_load(own * chunks + k, k % SLOTS).wait()
        wt[k] = w0buf[k % SLOTS].T
        return carry

    lax.fori_loop(0, chunks, keep, 0)
    for_ship(lambda where: ship(where).wait())
    r_spread(0)

    def w_store(ref, first, n, k):
        rows = pl.ds(pl.multiple_of(k * CHUNK, CHUNK), CHUNK)
        slot = (first + k) % SLOTS
        return pltpu.make_async_copy(w0buf.at[slot], ref.at[rows, :], out_sem.at[slot])

    def w_copy(k):
        rows = pl.ds(pl.multiple_of(k * CHUNK, CHUNK), CHUNK)
        slot = k % SLOTS
        return pltpu.make_async_remote_copy(
            src_ref=w0buf.at[slot], dst_ref=w_far.at[rows, :], send_sem=w_send.at[slot], recv_sem=w_recv.at[slot],
            device_id=partner_id, device_id_type=MESH)

    def w_out():
        first = 0
        for ref, n in (*zip(w_pieces, PIECES), (w_near, KEPT)):

            def put(k, carry, ref=ref, n=n, first=first):
                chunk = first + k
                slot = chunk % SLOTS

                @pl.when(chunk >= SLOTS)
                def _():
                    w_store(ref, first, n, k).wait()

                w0buf[slot] = wt[chunk].T
                w_store(ref, first, n, k).start()
                return carry

            lax.fori_loop(0, n, put, 0)
            first += n

        def send(k, carry):
            w_copy(k).start()
            return carry

        lax.fori_loop(0, KEPT, send, 0)

    def sweep(t, carry):
        parity = (t + 1) % 2
        more = t < SWEEPS - 1
        at = t * (6 * chunks + 2)
        own_columns(0, t, at, own_load)
        r_spread(1)
        own_columns(1, t, at + chunks + 1, other_load)

        @pl.when(jnp.logical_not(more))
        def _():
            w_out()

        at = at + 2 * chunks + 2
        partner_columns(0, at, other_load)
        u_begin(parity, 0)
        u_end(parity, 0)

        @pl.when(more)
        def _():
            r_begin(0)
            partner_gradient(0, at, other_load)

        partner_columns(1, at, other_load, more)

        @pl.when(more)
        def _():
            r_spread(0)

        u_begin(parity, 1)
        u_end(parity, 1)

        @pl.when(more)
        def _():
            r_begin(1)
            partner_gradient(1, at, own_load)

        return carry

    lax.fori_loop(0, SWEEPS, sweep, 0)
    r_stores = []
    for i in range(2):
        w0buf[SLOTS + i] = rt[:, i * CHUNK:(i + 1) * CHUNK].T
        r_stores.append(
            pltpu.make_async_copy(w0buf.at[SLOTS + i], r_hbm.at[pl.ds(i * CHUNK, CHUNK), :], in_sem.at[i]))
        r_stores[i].start()

    def drain(k, carry):
        for g in range(len(GROUPS)):
            s_copy(g, k).wait_send()
        return carry

    lax.fori_loop(0, chunks, drain, 0)
    for k in range(KEPT):
        w_store(w_near, sum(PIECES), KEPT, k).wait()
        w_copy(k).wait()
    for store in r_stores:
        store.wait()


def place(result, piece, half, first, shape, extra=None):
    rows, width = piece.shape
    halves = shape[0] // CHUNK // 2
    here = pl.BlockSpec((CHUNK, width), lambda i, half_ref: (half_ref[0] * halves + first + i, 0))
    out_shape, out_specs = [jax.ShapeDtypeStruct(shape, piece.dtype)], [here]

    def body(half_ref, piece_ref, other_ref, out_ref, *copied):
        out_ref[...] = piece_ref[...]
        for ref in copied:
            ref[...] = other_ref[...]

    if result is None:
        whole = pl.BlockSpec(extra.shape, lambda i, half_ref: (0, 0))
        out_shape.append(jax.ShapeDtypeStruct(extra.shape, extra.dtype))
        out_specs.append(whole)
        other, other_spec, aliases = extra, whole, {}
    else:
        other, other_spec, aliases = result, pl.BlockSpec(memory_space=pl.ANY), {2: 0}
    return pl.pallas_call(
        body,
        name="place",
        out_shape=out_shape,
        grid_spec=pltpu.PrefetchScalarGridSpec(
            num_scalar_prefetch=1,
            grid=(rows // CHUNK,),
            in_specs=[pl.BlockSpec((CHUNK, width), lambda i, half_ref: (i, 0)), other_spec],
            out_specs=out_specs,
        ),
        input_output_aliases=aliases,
    )(half, piece, other)


def solution(mesh):
    samp_size = mesh.shape["samp"]
    design_spec = P(("problem", "samp"), "feat")
    rows_spec = P(("problem", "samp"), None)
    coef_spec = P(("problem", "feat"), None)
    step_spec = P(("problem", "feat"))
    ridge_spec = P("problem")

    def local_sweeps(design, targets, coef_init, step_sizes, ridge_weights):
        rows, columns = design.shape
        width = targets.shape[1]
        groups = len(GROUPS)
        chunks = columns // CHUNK // samp_size
        bf16, f32 = jnp.bfloat16, jnp.float32
        vmem, dma = pltpu.VMEM, pltpu.SemaphoreType.DMA
        in_hbm = pl.BlockSpec(memory_space=pltpu.HBM)
        sizes = (KEPT, KEPT, *PIECES)
        resid, _, near, far, *pieces = pl.pallas_call(
            functools.partial(sweep_kernel, rows * samp_size),
            name="sweeps",
            out_shape=(
                jax.ShapeDtypeStruct((rows, width), f32),
                jax.ShapeDtypeStruct((rows, EXTRA + SHIPPED), bf16),
                *(jax.ShapeDtypeStruct((n * CHUNK, width), f32) for n in sizes),
            ),
            in_specs=[in_hbm] * 5,
            out_specs=(in_hbm,) * (2 + len(sizes)),
            scratch_shapes=[
                vmem((SLOTS, rows, CHUNK), bf16),
                vmem((2, CHUNK, rows // ROW_BLOCKS), bf16),
                vmem((SLOTS + 2, CHUNK, width), f32),
                vmem((chunks, width, CHUNK), f32),
                vmem((chunks, width, CHUNK), f32),
                vmem((2 * chunks, width, CHUNK), bf16),
                vmem((chunks, width, CHUNK), f32),
                vmem((width, rows), f32),
                vmem((width, rows // ROW_BLOCKS), f32),
                vmem((width, rows), f32),
                vmem((width, rows), bf16),
                vmem((width, rows), bf16),
                vmem((2, 4, width, rows), bf16),
                vmem((columns // 128, 128), f32),
                vmem((1, width), f32),
                vmem((width, width), f32),
                dma((SLOTS, ROW_BLOCKS)),
                dma((SLOTS + 2,)),
                dma((2,)),
                dma((2,)),
                dma((groups, 4)),
                dma((groups, 4)),
                dma((groups, chunks)),
                dma((groups, chunks)),
                dma((groups, chunks)),
                dma((groups, chunks)),
                dma((ROW_BLOCKS, groups, 3)),
                dma((ROW_BLOCKS, groups, 3)),
                dma((2, groups, 3)),
                dma((2, groups, 3)),
                dma((SLOTS,)),
                dma((SLOTS,)),
                dma((SLOTS,)),
            ],
            compiler_params=pltpu.CompilerParams(
                collective_id=0, has_side_effects=True, vmem_limit_bytes=67_000_000),
        )(design, targets, coef_init, step_sizes.reshape(columns // 128, 128), ridge_weights.reshape(1, width))
        here = lax.axis_index("samp").astype(jnp.int32).reshape(1)
        swap = [(i, samp_size - 1 - i) for i in range(samp_size)]
        arrived = [lax.ppermute(piece, "samp", swap) for piece in pieces]
        shape = (columns, width)
        coef, resid = place(None, near, here, sum(PIECES), shape, resid)
        for half, parts in ((here, pieces), (1 - here, arrived)):
            first = 0
            for piece, n in zip(parts, PIECES):
                (coef,) = place(coef, piece, half, first, shape)
                if half is here and first == 0:
                    (coef,) = place(coef, far, 1 - here, sum(PIECES), shape)
                first += n
        return coef, resid

    return jax.shard_map(
        local_sweeps, mesh=mesh, in_specs=(design_spec, rows_spec, coef_spec, step_spec, ridge_spec),
        out_specs=(coef_spec, rows_spec), check_vma=False)
```

```python
import functools

import jax
import jax.numpy as jnp
from jax import lax
from jax.experimental import pallas as pl
from jax.experimental.pallas import tpu as pltpu
from jax.sharding import PartitionSpec as P

SWEEPS = 4
STEP_WEIGHT = 0.5
CHUNK = 1024
SLOTS = 4
GROUPS = ((0, 48), (48, 80))
SHIPPED = 512
EXTRA = 128
ROW_BLOCKS = 4
KEPT = 4
PIECES = (6, 5, 1)
MESH = pl.DeviceIdType.MESH


def dot_t(left, right):
    return lax.dot_general(left, right, (((1,), (1,)), ((), ())), preferred_element_type=jnp.float32)


def sweep_kernel(
    total_rows, x_hbm, y_hbm, w0_hbm, eta_hbm, lam_hbm,
    r_hbm, shipped_hbm, w_near, w_far, *rest,
):
    w_pieces, rest = rest[: len(PIECES)], rest[len(PIECES):]
    (
        xbuf, turned, w0buf, gsend, grecv, sbuf, wt, ut, acc, rt, rbt, ra, uall, eta_ref, lam_ref, lam_col,
        x_sem, w0_sem, in_sem, ship_sem, r_send, r_recv, g_send, g_recv, s_send, s_recv, f_send, f_recv, u_send, u_recv, w_send, w_recv, out_sem, turn_sem,
    ) = rest
    z, s, f = lax.axis_index("problem"), lax.axis_index("samp"), lax.axis_index("feat")
    chunks, targets, _ = wt.shape
    core, chip = f % 2, f // 2
    near = chip * 2 + (1 - core)
    far = (1 - chip) * 2 + core
    partner_id = (z, 1 - s, f)
    near_id, far_id = (z, s, near), (z, s, far)
    own, other = s, 1 - s

    barrier = pltpu.get_barrier_semaphore()
    for device in (partner_id, near_id, far_id):
        pl.semaphore_signal(barrier, inc=1, device_id=device, device_id_type=MESH)

    def columns_of(chunk):
        return pl.ds(pl.multiple_of(chunk * CHUNK, CHUNK), CHUNK)

    def x_load(chunk, slot):
        return pltpu.make_async_copy(x_hbm.at[:, columns_of(chunk)], xbuf.at[slot], x_sem.at[slot, 0])

    def w0_load(chunk, slot):
        return pltpu.make_async_copy(w0_hbm.at[columns_of(chunk), :], w0buf.at[slot], w0_sem.at[slot])

    def part(ref, g, k):
        return ref.at[k, pl.ds(*GROUPS[g]), :]

    def rows_of(g):
        return pl.ds(*GROUPS[g])

    def g_copy(g, k):
        return pltpu.make_async_remote_copy(
            src_ref=part(gsend, g, k), dst_ref=part(grecv, g, k), send_sem=g_send.at[g, k], recv_sem=g_recv.at[g, k],
            device_id=partner_id, device_id_type=MESH)

    def s_copy(g, k):
        return pltpu.make_async_remote_copy(
            src_ref=part(sbuf, g, k), dst_ref=part(sbuf, g, chunks + k), send_sem=s_send.at[g, k], recv_sem=s_recv.at[g, k],
            device_id=partner_id, device_id_type=MESH)

    def u_copy(parity, g, slot, which, device):
        rows = uall.at[parity, slot, rows_of(g), :]
        return pltpu.make_async_remote_copy(
            src_ref=rows, dst_ref=rows,
            send_sem=u_send.at[parity, g, which], recv_sem=u_recv.at[parity, g, which],
            device_id=device, device_id_type=MESH)

    ahead = SLOTS - 1

    def start(copy):
        copy.start(priority=1)

    def wait(copy):
        copy.wait()

    def other_load(i, slot, act):
        act(x_load(other * chunks + i, slot))

    def for_ship(act):
        @pl.when(core == 0)
        def _():
            act(pl.ds(0, EXTRA + SHIPPED))

        @pl.when(core == 1)
        def _():
            act(pl.ds(EXTRA, SHIPPED))

    def own_load(i, slot, act):
        @pl.when(i != chunks - 1)
        def _():
            act(x_load(own * chunks + i - i // chunks, slot))

        @pl.when(i == chunks - 1)
        def _():
            for_ship(
                lambda where: act(
                    pltpu.make_async_copy(shipped_hbm.at[:, where], xbuf.at[slot, :, where], x_sem.at[slot, 0])))

    def steps(base, count, load, next_load, body, more=None):
        def step(i, carry):
            upcoming = i + ahead
            slot = (base + upcoming) % SLOTS

            @pl.when(upcoming < count)
            def _():
                load(upcoming, slot, start)

            wanted = upcoming >= count
            if more is not None:
                wanted = jnp.logical_and(wanted, more)

            @pl.when(wanted)
            def _():
                next_load(upcoming - count, slot, start)

            load(i, (base + i) % SLOTS, wait)
            body(i, (base + i) % SLOTS)
            return carry

        lax.fori_loop(0, count, step, 0)

    rows = x_hbm.shape[0] // ROW_BLOCKS
    width = xbuf.shape[1] // rows
    passes = 2 * chunks // width
    blocks = ROW_BLOCKS * passes
    pairs = w0buf.shape[0] // 2

    def tile_load(step, q):
        slot = step % SLOTS
        where = pl.ds(pl.multiple_of(step // passes * rows, rows), rows)
        return pltpu.make_async_copy(
            x_hbm.at[where, columns_of(step % passes * width + q)], xbuf.at[slot, pl.ds(q * rows, rows), :], x_sem.at[slot, q])

    def tiles_ahead(step):
        upcoming = step + ahead

        @pl.when(upcoming < blocks)
        def _():
            for q in range(width):
                tile_load(upcoming, q).start(priority=1)

        @pl.when(upcoming >= blocks)
        def _():
            x_load(other * chunks + upcoming - blocks, upcoming % SLOTS).start(priority=1)

    def w0_pair(pair, q):
        return w0_load(2 * pair + q, 2 * (pair % pairs) + q)

    eta_load = pltpu.make_async_copy(eta_hbm, eta_ref, in_sem.at[0])
    lam_load = pltpu.make_async_copy(lam_hbm, lam_ref, in_sem.at[1])
    halves = [
        pltpu.make_async_copy(
            y_hbm.at[pl.ds(i * CHUNK, CHUNK), :], w0buf.at[2 * pairs - 2 + i], w0_sem.at[2 * pairs - 2 + i])
        for i in range(2)
    ]
    for load in (*halves, lam_load, eta_load):
        load.start()
    for pair in range(pairs - 1):
        for q in range(2):
            w0_pair(pair, q).start()
    for step in range(ahead):
        for q in range(width):
            tile_load(step, q).start(priority=1)
    pl.semaphore_wait(barrier, 3)

    def ship(where):
        first = (other + 1) * chunks * CHUNK - EXTRA - SHIPPED + where.start
        return pltpu.make_async_remote_copy(
            src_ref=x_hbm.at[:, pl.ds(pl.multiple_of(first, 128), where.size)], dst_ref=shipped_hbm.at[:, where],
            send_sem=ship_sem.at[0], recv_sem=ship_sem.at[1], device_id=partner_id, device_id_type=MESH)

    for_ship(lambda where: ship(where).start())
    ut[...] = jnp.zeros_like(ut)
    acc[...] = jnp.zeros_like(acc)
    for i, load in enumerate(halves):
        load.wait()
        rt[:, i * CHUNK:(i + 1) * CHUNK] = w0buf[2 * pairs - 2 + i].T
    lam_load.wait()
    lam_col[...] = jnp.broadcast_to(lam_ref[0:1, :], (targets, targets)).T

    def first_pass(pair, carry):
        @pl.when(pair % (width // 2) == 0)
        def _():
            tiles_ahead(pair // (width // 2))

        @pl.when(pair + pairs - 1 < chunks)
        def _():
            for q in range(2):
                w0_pair(pair + pairs - 1, q).start()

        slot = pair // (width // 2) % SLOTS
        first = pair % (width // 2) * 2
        total = acc[...]
        for q in range(2):
            w0_pair(pair, q).wait()
            tile_load(pair // (width // 2), first + q).wait()
        for q in range(2):
            weights = w0buf[2 * (pair % pairs) + q].T.astype(jnp.bfloat16)
            sbuf[2 * pair + q] = weights
            where = pl.ds(pl.multiple_of((first + q) * rows, rows), rows)
            total += dot_t(weights, xbuf[slot, where, :])
        acc[...] = total
        return carry

    def block_product(weights, tiles):
        plain = len(tiles) // 2
        for q, tile in enumerate(tiles[plain:]):
            turned[q] = tile.T
        total = sum(dot_t(weight, tile) for weight, tile in zip(weights[:plain], tiles))
        for q, weight in enumerate(weights[plain:]):
            total += jnp.dot(weight, turned[q], preferred_element_type=jnp.float32)
        return total

    def later_pass(block, carry):
        def step_(i, inner):
            step = block * passes + i
            tiles_ahead(step)
            for q in range(width):
                tile_load(step, q).wait()
            slot = step % SLOTS
            acc[...] += block_product(
                [sbuf[i * width + q] for q in range(width)],
                [xbuf[slot, q * rows:(q + 1) * rows, :] for q in range(width)])
            return inner

        lax.fori_loop(0, passes, step_, 0)
        return carry

    def lanes_of(block):
        return pl.ds(block * rows, rows)

    def first_copy(block, g, slot, which, device):
        ref = uall.at[0, slot, rows_of(g), lanes_of(block)]
        return pltpu.make_async_remote_copy(
            src_ref=ref, dst_ref=ref, send_sem=f_send.at[block, g, which], recv_sem=f_recv.at[block, g, which],
            device_id=device, device_id_type=MESH)

    def first_begin(block):
        uall[0, f, :, lanes_of(block)] = acc[...].astype(jnp.bfloat16)
        acc[...] = jnp.zeros_like(acc)
        for g in range(len(GROUPS)):
            first_copy(block, g, f, 0, near_id).start()
            first_copy(block, g, f, 1, far_id).start()

    def first_forward(block, g):
        first_copy(block, g, far, 1, far_id).wait_recv()
        first_copy(block, g, far, 2, near_id).start()

    def first_end(block, g):
        first_copy(block, g, near, 0, near_id).wait_recv()
        first_copy(block, g, far, 2, near_id).wait_recv()
        total = uall[0, 0, rows_of(g), lanes_of(block)].astype(jnp.float32)
        for j in range(1, 4):
            total += uall[0, j, rows_of(g), lanes_of(block)].astype(jnp.float32)
        new = rt[rows_of(g), lanes_of(block)] - total
        rt[rows_of(g), lanes_of(block)] = new
        rbt[rows_of(g), lanes_of(block)] = new.astype(jnp.bfloat16)
        first_copy(block, g, f, 0, near_id).wait_send()
        first_copy(block, g, f, 1, far_id).wait_send()
        first_copy(block, g, far, 2, near_id).wait_send()

    lax.fori_loop(0, chunks, first_pass, 0)
    last = ROW_BLOCKS - 1
    for block in range(ROW_BLOCKS):
        if block:
            later_pass(block, 0)
        first_begin(block)
        for g in range(len(GROUPS)):
            if block >= 1:
                first_forward(block - 1, g)
            if block >= 2:
                first_end(block - 2, g)

    def u_begin(parity, g):
        uall[parity, f, rows_of(g), :] = ut[rows_of(g), :].astype(jnp.bfloat16)
        ut[rows_of(g), :] = jnp.zeros((GROUPS[g][1], ut.shape[1]), jnp.float32)
        u_copy(parity, g, f, 0, near_id).start()
        u_copy(parity, g, f, 1, far_id).start()

    def u_end(parity, g):
        u_copy(parity, g, far, 1, far_id).wait_recv()
        u_copy(parity, g, far, 2, near_id).start()
        u_copy(parity, g, near, 0, near_id).wait_recv()
        u_copy(parity, g, far, 2, near_id).wait_recv()
        total = uall[parity, 0, rows_of(g), :].astype(jnp.float32)
        for block in range(1, 4):
            total += uall[parity, block, rows_of(g), :].astype(jnp.float32)
        new = rt[rows_of(g), :] - STEP_WEIGHT * total
        rt[rows_of(g), :] = new
        rbt[rows_of(g), :] = new.astype(jnp.bfloat16)
        u_copy(parity, g, f, 0, near_id).wait_send()
        u_copy(parity, g, f, 1, far_id).wait_send()
        u_copy(parity, g, far, 2, near_id).wait_send()

    quarter = ra.shape[1] // 4

    def r_copy(g, source, of, which, device):
        lanes = pl.ds(pl.multiple_of(of * quarter, quarter), quarter)
        return pltpu.make_async_remote_copy(
            src_ref=source.at[rows_of(g), lanes], dst_ref=ra.at[rows_of(g), lanes],
            send_sem=r_send.at[g, which], recv_sem=r_recv.at[g, which], device_id=device, device_id_type=MESH)

    def r_begin(g):
        r_copy(g, rbt, f, 0, partner_id).start()

    def r_spread(g):
        r_copy(g, rbt, f, 0, partner_id).wait()
        r_copy(g, ra, f, 1, near_id).start()
        r_copy(g, ra, f, 2, far_id).start()

    def r_end(g):
        r_copy(g, ra, far, 2, far_id).wait_recv()
        r_copy(g, ra, far, 3, near_id).start()
        r_copy(g, ra, near, 1, near_id).wait_recv()
        r_copy(g, ra, far, 3, near_id).wait_recv()
        r_copy(g, ra, f, 1, near_id).wait_send()
        r_copy(g, ra, f, 2, far_id).wait_send()
        r_copy(g, ra, far, 3, near_id).wait_send()

    sent = CHUNK - SHIPPED

    def last_copy(g, size):
        lanes = pl.ds(0, size)
        return pltpu.make_async_remote_copy(
            src_ref=gsend.at[chunks - 1, rows_of(g), lanes], dst_ref=grecv.at[chunks - 1, rows_of(g), lanes],
            send_sem=g_send.at[g, chunks - 1], recv_sem=g_recv.at[g, chunks - 1],
            device_id=partner_id, device_id_type=MESH)

    def for_g_copy(g, k, act):
        @pl.when(k < chunks - 1)
        def _():
            act(g_copy(g, k))

        for which, size in enumerate((sent - EXTRA, sent)):

            @pl.when(jnp.logical_and(k == chunks - 1, core == which))
            def _(size=size):
                act(last_copy(g, size))

    def partner_gradient(g, base, next_load):
        def body(k, slot):
            gsend[k, rows_of(g), :] = jnp.dot(rbt[rows_of(g), :], xbuf[slot], preferred_element_type=jnp.float32)
            for_g_copy(g, k, lambda copy: copy.start())

        steps(base, chunks, other_load, next_load, body)

    def own_columns(g, t, base, next_load):
        lam = lam_col[rows_of(g), 0:1]

        def body(i, slot):
            @pl.when(i == chunks - 1)
            def _():
                r_end(g)
                grecv[chunks - 1, rows_of(g), sent:] = jnp.dot(
                    ra[rows_of(g), :], xbuf[slot, :, EXTRA:EXTRA + SHIPPED], preferred_element_type=jnp.float32)

                @pl.when(core == 0)
                def _():
                    grecv[chunks - 1, rows_of(g), sent - EXTRA:sent] = jnp.dot(
                        ra[rows_of(g), :], xbuf[slot, :, 0:EXTRA], preferred_element_type=jnp.float32)

            @pl.when(i != chunks - 1)
            def _():
                k = i - i // chunks
                for_g_copy(g, k, lambda copy: copy.wait_recv())

                @pl.when(t > 0)
                def _():
                    s_copy(g, k).wait_send()

                mine = jnp.dot(rbt[rows_of(g), :], xbuf[slot], preferred_element_type=jnp.float32)
                weights = wt[k, rows_of(g), :]
                gradient = (mine + grecv[k, rows_of(g), :]) * (1.0 / total_rows)
                lanes = eta_ref.shape[1]
                first = (own * chunks + k) * (CHUNK // lanes)
                eta = jnp.concatenate([eta_ref[pl.ds(first + j, 1), :] for j in range(CHUNK // lanes)], axis=1)
                delta = eta * (gradient - lam * weights)
                wt[k, rows_of(g), :] = weights + STEP_WEIGHT * delta
                delta_b = delta.astype(jnp.bfloat16)
                sbuf[k, rows_of(g), :] = delta_b
                ut[rows_of(g), :] += dot_t(delta_b, xbuf[slot])
                s_copy(g, k).start()

        steps(base, chunks + 1, own_load, next_load, body)

    def partner_columns(g, base, next_load, more=None):
        def body(k, slot):
            s_copy(g, k).wait_recv()
            for_g_copy(g, k, lambda copy: copy.wait_send())
            ut[rows_of(g), :] += dot_t(sbuf[chunks + k, rows_of(g), :], xbuf[slot])

        steps(base, chunks, other_load, next_load, body, more)

    first_forward(last, 0)
    first_end(last - 1, 0)
    first_end(last, 0)
    r_begin(0)
    first_forward(last, 1)
    partner_gradient(0, blocks, other_load)
    first_end(last - 1, 1)
    first_end(last, 1)
    r_begin(1)
    partner_gradient(1, blocks, own_load)

    eta_load.wait()
    for k in range(ahead):
        w0_load(own * chunks + k, k).start()

    def keep(k, carry):
        @pl.when(k + ahead < chunks)
        def _():
            w0_load(own * chunks + k + ahead, (k + ahead) % SLOTS).start()

        w0_load(own * chunks + k, k % SLOTS).wait()
        wt[k] = w0buf[k % SLOTS].T
        return carry

    lax.fori_loop(0, chunks, keep, 0)
    for_ship(lambda where: ship(where).wait())
    r_spread(0)

    def w_store(ref, first, n, k):
        rows = pl.ds(pl.multiple_of(k * CHUNK, CHUNK), CHUNK)
        slot = (first + k) % SLOTS
        return pltpu.make_async_copy(w0buf.at[slot], ref.at[rows, :], out_sem.at[slot])

    def w_copy(k):
        rows = pl.ds(pl.multiple_of(k * CHUNK, CHUNK), CHUNK)
        slot = k % SLOTS
        return pltpu.make_async_remote_copy(
            src_ref=w0buf.at[slot], dst_ref=w_far.at[rows, :], send_sem=w_send.at[slot], recv_sem=w_recv.at[slot],
            device_id=partner_id, device_id_type=MESH)

    def w_send_all():
        for k in range(KEPT):
            w_copy(k).start()

    def w_out():
        first = 0
        for ref, n in (*zip(w_pieces, PIECES), (w_near, KEPT)):

            def put(k, carry, ref=ref, n=n, first=first):
                chunk = first + k
                slot = chunk % SLOTS

                @pl.when(chunk >= SLOTS)
                def _():
                    w_store(ref, first, n, k).wait()

                w0buf[slot] = wt[chunk].T
                w_store(ref, first, n, k).start()
                return carry

            lax.fori_loop(0, n, put, 0)
            first += n

        @pl.when(core == 0)
        def _():
            w_send_all()

    def sweep(t, carry):
        parity = (t + 1) % 2
        more = t < SWEEPS - 1
        at = t * (6 * chunks + 2)
        own_columns(0, t, at, own_load)
        r_spread(1)
        own_columns(1, t, at + chunks + 1, other_load)

        @pl.when(jnp.logical_not(more))
        def _():
            w_out()

        at = at + 2 * chunks + 2
        partner_columns(0, at, other_load)
        u_begin(parity, 0)
        u_end(parity, 0)

        @pl.when(more)
        def _():
            r_begin(0)
            partner_gradient(0, at, other_load)

        partner_columns(1, at, other_load, more)

        @pl.when(more)
        def _():
            r_spread(0)

        u_begin(parity, 1)
        u_end(parity, 1)

        @pl.when(more)
        def _():
            r_begin(1)
            partner_gradient(1, at, own_load)

        return carry

    lax.fori_loop(0, SWEEPS, sweep, 0)
    r_stores = []
    for i in range(2):
        w0buf[SLOTS + i] = rt[:, i * CHUNK:(i + 1) * CHUNK].T
        r_stores.append(
            pltpu.make_async_copy(w0buf.at[SLOTS + i], r_hbm.at[pl.ds(i * CHUNK, CHUNK), :], in_sem.at[i]))
        r_stores[i].start()

    @pl.when(core == 0)
    def _():
        for k in range(KEPT - 1):
            w_copy(k).wait_send()
        pl.semaphore_signal(turn_sem, inc=1, device_id=near_id, device_id_type=MESH)
        w_copy(KEPT - 1).wait_send()

    @pl.when(core == 1)
    def _():
        pl.semaphore_wait(turn_sem, 1)
        w_send_all()
        for k in range(KEPT):
            w_copy(k).wait_send()


    def drain(k, carry):
        for g in range(len(GROUPS)):
            s_copy(g, k).wait_send()
        return carry

    lax.fori_loop(0, chunks, drain, 0)
    for k in range(KEPT):
        w_store(w_near, sum(PIECES), KEPT, k).wait()
        w_copy(k).wait_recv()
    for store in r_stores:
        store.wait()


def place(result, piece, half, first, shape, extra=None):
    rows, width = piece.shape
    halves = shape[0] // CHUNK // 2
    here = pl.BlockSpec((CHUNK, width), lambda i, half_ref: (half_ref[0] * halves + first + i, 0))
    out_shape, out_specs = [jax.ShapeDtypeStruct(shape, piece.dtype)], [here]

    def body(half_ref, piece_ref, other_ref, out_ref, *copied):
        out_ref[...] = piece_ref[...]
        for ref in copied:
            ref[...] = other_ref[...]

    if result is None:
        whole = pl.BlockSpec(extra.shape, lambda i, half_ref: (0, 0))
        out_shape.append(jax.ShapeDtypeStruct(extra.shape, extra.dtype))
        out_specs.append(whole)
        other, other_spec, aliases = extra, whole, {}
    else:
        other, other_spec, aliases = result, pl.BlockSpec(memory_space=pl.ANY), {2: 0}
    return pl.pallas_call(
        body,
        name="place",
        out_shape=out_shape,
        grid_spec=pltpu.PrefetchScalarGridSpec(
            num_scalar_prefetch=1,
            grid=(rows // CHUNK,),
            in_specs=[pl.BlockSpec((CHUNK, width), lambda i, half_ref: (i, 0)), other_spec],
            out_specs=out_specs,
        ),
        input_output_aliases=aliases,
    )(half, piece, other)


def solution(mesh):
    samp_size = mesh.shape["samp"]
    design_spec = P(("problem", "samp"), "feat")
    rows_spec = P(("problem", "samp"), None)
    coef_spec = P(("problem", "feat"), None)
    step_spec = P(("problem", "feat"))
    ridge_spec = P("problem")

    def local_sweeps(design, targets, coef_init, step_sizes, ridge_weights):
        rows, columns = design.shape
        width = targets.shape[1]
        groups = len(GROUPS)
        chunks = columns // CHUNK // samp_size
        bf16, f32 = jnp.bfloat16, jnp.float32
        vmem, dma = pltpu.VMEM, pltpu.SemaphoreType.DMA
        in_hbm = pl.BlockSpec(memory_space=pltpu.HBM)
        sizes = (KEPT, KEPT, *PIECES)
        resid, _, near, far, *pieces = pl.pallas_call(
            functools.partial(sweep_kernel, rows * samp_size),
            name="sweeps",
            out_shape=(
                jax.ShapeDtypeStruct((rows, width), f32),
                jax.ShapeDtypeStruct((rows, EXTRA + SHIPPED), bf16),
                *(jax.ShapeDtypeStruct((n * CHUNK, width), f32) for n in sizes),
            ),
            in_specs=[in_hbm] * 5,
            out_specs=(in_hbm,) * (2 + len(sizes)),
            scratch_shapes=[
                vmem((SLOTS, rows, CHUNK), bf16),
                vmem((2, CHUNK, rows // ROW_BLOCKS), bf16),
                vmem((SLOTS + 2, CHUNK, width), f32),
                vmem((chunks, width, CHUNK), f32),
                vmem((chunks, width, CHUNK), f32),
                vmem((2 * chunks, width, CHUNK), bf16),
                vmem((chunks, width, CHUNK), f32),
                vmem((width, rows), f32),
                vmem((width, rows // ROW_BLOCKS), f32),
                vmem((width, rows), f32),
                vmem((width, rows), bf16),
                vmem((width, rows), bf16),
                vmem((2, 4, width, rows), bf16),
                vmem((columns // 128, 128), f32),
                vmem((1, width), f32),
                vmem((width, width), f32),
                dma((SLOTS, ROW_BLOCKS)),
                dma((SLOTS + 2,)),
                dma((2,)),
                dma((2,)),
                dma((groups, 4)),
                dma((groups, 4)),
                dma((groups, chunks)),
                dma((groups, chunks)),
                dma((groups, chunks)),
                dma((groups, chunks)),
                dma((ROW_BLOCKS, groups, 3)),
                dma((ROW_BLOCKS, groups, 3)),
                dma((2, groups, 3)),
                dma((2, groups, 3)),
                dma((SLOTS,)),
                dma((SLOTS,)),
                dma((SLOTS,)),
                pltpu.SemaphoreType.REGULAR,
            ],
            compiler_params=pltpu.CompilerParams(
                collective_id=0, has_side_effects=True, vmem_limit_bytes=67_000_000),
        )(design, targets, coef_init, step_sizes.reshape(columns // 128, 128), ridge_weights.reshape(1, width))
        here = lax.axis_index("samp").astype(jnp.int32).reshape(1)
        swap = [(i, samp_size - 1 - i) for i in range(samp_size)]
        arrived = [lax.ppermute(piece, "samp", swap) for piece in pieces]
        shape = (columns, width)
        coef, resid = place(None, near, here, sum(PIECES), shape, resid)
        for half, parts in ((here, pieces), (1 - here, arrived)):
            first = 0
            for piece, n in zip(parts, PIECES):
                (coef,) = place(coef, piece, half, first, shape)
                if half is here and first == 0:
                    (coef,) = place(coef, far, 1 - here, sum(PIECES), shape)
                first += n
        return coef, resid

    return jax.shard_map(
        local_sweeps, mesh=mesh, in_specs=(design_spec, rows_spec, coef_spec, step_spec, ridge_spec),
        out_specs=(coef_spec, rows_spec), check_vma=False)
```

```python
import functools

import jax
import jax.numpy as jnp
from jax import lax
from jax.experimental import pallas as pl
from jax.experimental.pallas import tpu as pltpu
from jax.sharding import PartitionSpec as P

SWEEPS = 4
STEP_WEIGHT = 0.5
CHUNK = 1024
SLOTS = 4
GROUPS = ((0, 48), (48, 80))
SHIPPED = 512
EXTRA = 128
ROW_BLOCKS = 4
KEPT = 4
PIECES = (6, 5, 1)
MESH = pl.DeviceIdType.MESH


def dot_t(left, right):
    return lax.dot_general(left, right, (((1,), (1,)), ((), ())), preferred_element_type=jnp.float32)


def sweep_kernel(
    total_rows, x_hbm, y_hbm, w0_hbm, eta_hbm, lam_hbm,
    r_hbm, shipped_hbm, w_near, w_far, *rest,
):
    w_pieces, rest = rest[: len(PIECES)], rest[len(PIECES):]
    (
        xbuf, turned, w0buf, gsend, grecv, sbuf, wt, ut, acc, rt, rbt, ra, uall, eta_ref, lam_ref, lam_col,
        x_sem, w0_sem, in_sem, ship_sem, r_send, r_recv, g_send, g_recv, s_send, s_recv, f_send, f_recv, u_send, u_recv, w_send, w_recv, out_sem, turn_sem,
    ) = rest
    z, s, f = lax.axis_index("problem"), lax.axis_index("samp"), lax.axis_index("feat")
    chunks, targets, _ = wt.shape
    core, chip = f % 2, f // 2
    near = chip * 2 + (1 - core)
    far = (1 - chip) * 2 + core
    partner_id = (z, 1 - s, f)
    near_id, far_id = (z, s, near), (z, s, far)
    own, other = s, 1 - s

    barrier = pltpu.get_barrier_semaphore()
    for device in (partner_id, near_id, far_id):
        pl.semaphore_signal(barrier, inc=1, device_id=device, device_id_type=MESH)

    def columns_of(chunk):
        return pl.ds(pl.multiple_of(chunk * CHUNK, CHUNK), CHUNK)

    def x_load(chunk, slot):
        return pltpu.make_async_copy(x_hbm.at[:, columns_of(chunk)], xbuf.at[slot], x_sem.at[slot, 0])

    def w0_load(chunk, slot):
        return pltpu.make_async_copy(w0_hbm.at[columns_of(chunk), :], w0buf.at[slot], w0_sem.at[slot])

    def part(ref, g, k):
        return ref.at[k, pl.ds(*GROUPS[g]), :]

    def rows_of(g):
        return pl.ds(*GROUPS[g])

    def g_copy(g, k):
        return pltpu.make_async_remote_copy(
            src_ref=part(gsend, g, k), dst_ref=part(grecv, g, k), send_sem=g_send.at[g, k], recv_sem=g_recv.at[g, k],
            device_id=partner_id, device_id_type=MESH)

    def s_copy(g, k):
        return pltpu.make_async_remote_copy(
            src_ref=part(sbuf, g, k), dst_ref=part(sbuf, g, chunks + k), send_sem=s_send.at[g, k], recv_sem=s_recv.at[g, k],
            device_id=partner_id, device_id_type=MESH)

    def u_copy(parity, g, slot, which, device):
        rows = uall.at[parity, slot, rows_of(g), :]
        return pltpu.make_async_remote_copy(
            src_ref=rows, dst_ref=rows,
            send_sem=u_send.at[parity, g, which], recv_sem=u_recv.at[parity, g, which],
            device_id=device, device_id_type=MESH)

    ahead = SLOTS - 1

    def start(copy):
        copy.start(priority=1)

    def wait(copy):
        copy.wait()

    def other_load(i, slot, act):
        act(x_load(other * chunks + i, slot))

    def for_ship(act):
        @pl.when(core == 0)
        def _():
            act(pl.ds(0, EXTRA + SHIPPED))

        @pl.when(core == 1)
        def _():
            act(pl.ds(EXTRA, SHIPPED))

    def own_load(i, slot, act):
        @pl.when(i != chunks - 1)
        def _():
            act(x_load(own * chunks + i - i // chunks, slot))

        @pl.when(i == chunks - 1)
        def _():
            for_ship(
                lambda where: act(
                    pltpu.make_async_copy(shipped_hbm.at[:, where], xbuf.at[slot, :, where], x_sem.at[slot, 0])))

    def steps(base, count, load, next_load, body, more=None):
        def step(i, carry):
            upcoming = i + ahead
            slot = (base + upcoming) % SLOTS

            @pl.when(upcoming < count)
            def _():
                load(upcoming, slot, start)

            wanted = upcoming >= count
            if more is not None:
                wanted = jnp.logical_and(wanted, more)

            @pl.when(wanted)
            def _():
                next_load(upcoming - count, slot, start)

            load(i, (base + i) % SLOTS, wait)
            body(i, (base + i) % SLOTS)
            return carry

        lax.fori_loop(0, count, step, 0)

    rows = x_hbm.shape[0] // ROW_BLOCKS
    width = xbuf.shape[1] // rows
    passes = 2 * chunks // width
    blocks = ROW_BLOCKS * passes
    pairs = w0buf.shape[0] // 2

    def tile_load(step, q):
        slot = step % SLOTS
        where = pl.ds(pl.multiple_of(step // passes * rows, rows), rows)
        return pltpu.make_async_copy(
            x_hbm.at[where, columns_of(step % passes * width + q)], xbuf.at[slot, pl.ds(q * rows, rows), :], x_sem.at[slot, q])

    def tiles_ahead(step):
        upcoming = step + ahead

        @pl.when(upcoming < blocks)
        def _():
            for q in range(width):
                tile_load(upcoming, q).start(priority=1)

        @pl.when(upcoming >= blocks)
        def _():
            x_load(other * chunks + upcoming - blocks, upcoming % SLOTS).start(priority=1)

    def w0_pair(pair, q):
        return w0_load(2 * pair + q, 2 * (pair % pairs) + q)

    eta_load = pltpu.make_async_copy(eta_hbm, eta_ref, in_sem.at[0])
    lam_load = pltpu.make_async_copy(lam_hbm, lam_ref, in_sem.at[1])
    halves = [
        pltpu.make_async_copy(
            y_hbm.at[pl.ds(i * CHUNK, CHUNK), :], w0buf.at[2 * pairs - 2 + i], w0_sem.at[2 * pairs - 2 + i])
        for i in range(2)
    ]
    for load in (*halves, lam_load, eta_load):
        load.start()
    for pair in range(pairs - 1):
        for q in range(2):
            w0_pair(pair, q).start()
    for step in range(ahead):
        for q in range(width):
            tile_load(step, q).start(priority=1)
    pl.semaphore_wait(barrier, 3)

    def ship(where):
        first = (other + 1) * chunks * CHUNK - EXTRA - SHIPPED + where.start
        return pltpu.make_async_remote_copy(
            src_ref=x_hbm.at[:, pl.ds(pl.multiple_of(first, 128), where.size)], dst_ref=shipped_hbm.at[:, where],
            send_sem=ship_sem.at[0], recv_sem=ship_sem.at[1], device_id=partner_id, device_id_type=MESH)

    for_ship(lambda where: ship(where).start())
    ut[...] = jnp.zeros_like(ut)
    acc[...] = jnp.zeros_like(acc)
    for i, load in enumerate(halves):
        load.wait()
        rt[:, i * CHUNK:(i + 1) * CHUNK] = w0buf[2 * pairs - 2 + i].T
    lam_load.wait()
    lam_col[...] = jnp.broadcast_to(lam_ref[0:1, :], (targets, targets)).T

    def first_pass(pair, carry):
        @pl.when(pair % (width // 2) == 0)
        def _():
            tiles_ahead(pair // (width // 2))

        @pl.when(pair + pairs - 1 < chunks)
        def _():
            for q in range(2):
                w0_pair(pair + pairs - 1, q).start()

        slot = pair // (width // 2) % SLOTS
        first = pair % (width // 2) * 2
        total = acc[...]
        for q in range(2):
            w0_pair(pair, q).wait()
            tile_load(pair // (width // 2), first + q).wait()
        for q in range(2):
            weights = w0buf[2 * (pair % pairs) + q].T.astype(jnp.bfloat16)
            sbuf[2 * pair + q] = weights
            where = pl.ds(pl.multiple_of((first + q) * rows, rows), rows)
            total += dot_t(weights, xbuf[slot, where, :])
        acc[...] = total
        return carry

    def block_product(weights, tiles):
        plain = len(tiles) // 2
        for q, tile in enumerate(tiles[plain:]):
            turned[q] = tile.T
        total = sum(dot_t(weight, tile) for weight, tile in zip(weights[:plain], tiles))
        for q, weight in enumerate(weights[plain:]):
            total += jnp.dot(weight, turned[q], preferred_element_type=jnp.float32)
        return total

    def later_pass(block, carry):
        def step_(i, inner):
            step = block * passes + i
            tiles_ahead(step)
            for q in range(width):
                tile_load(step, q).wait()
            slot = step % SLOTS
            acc[...] += block_product(
                [sbuf[i * width + q] for q in range(width)],
                [xbuf[slot, q * rows:(q + 1) * rows, :] for q in range(width)])
            return inner

        lax.fori_loop(0, passes, step_, 0)
        return carry

    def lanes_of(block):
        return pl.ds(block * rows, rows)

    def first_copy(block, g, slot, which, device):
        ref = uall.at[0, slot, rows_of(g), lanes_of(block)]
        return pltpu.make_async_remote_copy(
            src_ref=ref, dst_ref=ref, send_sem=f_send.at[block, g, which], recv_sem=f_recv.at[block, g, which],
            device_id=device, device_id_type=MESH)

    def first_begin(block):
        uall[0, f, :, lanes_of(block)] = acc[...].astype(jnp.bfloat16)
        acc[...] = jnp.zeros_like(acc)
        for g in range(len(GROUPS)):
            first_copy(block, g, f, 0, near_id).start()
            first_copy(block, g, f, 1, far_id).start()

    def first_forward(block, g):
        first_copy(block, g, far, 1, far_id).wait_recv()
        first_copy(block, g, far, 2, near_id).start()

    def first_end(block, g):
        first_copy(block, g, near, 0, near_id).wait_recv()
        first_copy(block, g, far, 2, near_id).wait_recv()
        total = uall[0, 0, rows_of(g), lanes_of(block)].astype(jnp.float32)
        for j in range(1, 4):
            total += uall[0, j, rows_of(g), lanes_of(block)].astype(jnp.float32)
        new = rt[rows_of(g), lanes_of(block)] - total
        rt[rows_of(g), lanes_of(block)] = new
        rbt[rows_of(g), lanes_of(block)] = new.astype(jnp.bfloat16)
        first_copy(block, g, f, 0, near_id).wait_send()
        first_copy(block, g, f, 1, far_id).wait_send()
        first_copy(block, g, far, 2, near_id).wait_send()

    lax.fori_loop(0, chunks, first_pass, 0)
    last = ROW_BLOCKS - 1
    for block in range(ROW_BLOCKS):
        if block:
            later_pass(block, 0)
        first_begin(block)
        for g in range(len(GROUPS)):
            if block >= 1:
                first_forward(block - 1, g)
            if block >= 2:
                first_end(block - 2, g)

    def u_begin(parity, g):
        uall[parity, f, rows_of(g), :] = ut[rows_of(g), :].astype(jnp.bfloat16)
        ut[rows_of(g), :] = jnp.zeros((GROUPS[g][1], ut.shape[1]), jnp.float32)
        u_copy(parity, g, f, 0, near_id).start()
        u_copy(parity, g, f, 1, far_id).start()

    def u_end(parity, g):
        u_copy(parity, g, far, 1, far_id).wait_recv()
        u_copy(parity, g, far, 2, near_id).start()
        u_copy(parity, g, near, 0, near_id).wait_recv()
        u_copy(parity, g, far, 2, near_id).wait_recv()
        total = uall[parity, 0, rows_of(g), :].astype(jnp.float32)
        for block in range(1, 4):
            total += uall[parity, block, rows_of(g), :].astype(jnp.float32)
        new = rt[rows_of(g), :] - STEP_WEIGHT * total
        rt[rows_of(g), :] = new
        rbt[rows_of(g), :] = new.astype(jnp.bfloat16)
        u_copy(parity, g, f, 0, near_id).wait_send()
        u_copy(parity, g, f, 1, far_id).wait_send()
        u_copy(parity, g, far, 2, near_id).wait_send()

    quarter = ra.shape[1] // 4

    def r_copy(g, source, of, which, device):
        lanes = pl.ds(pl.multiple_of(of * quarter, quarter), quarter)
        return pltpu.make_async_remote_copy(
            src_ref=source.at[rows_of(g), lanes], dst_ref=ra.at[rows_of(g), lanes],
            send_sem=r_send.at[g, which], recv_sem=r_recv.at[g, which], device_id=device, device_id_type=MESH)

    def r_begin(g):
        r_copy(g, rbt, f, 0, partner_id).start()

    def r_spread(g):
        r_copy(g, rbt, f, 0, partner_id).wait()
        r_copy(g, ra, f, 1, near_id).start()
        r_copy(g, ra, f, 2, far_id).start()

    def r_end(g):
        r_copy(g, ra, far, 2, far_id).wait_recv()
        r_copy(g, ra, far, 3, near_id).start()
        r_copy(g, ra, near, 1, near_id).wait_recv()
        r_copy(g, ra, far, 3, near_id).wait_recv()
        r_copy(g, ra, f, 1, near_id).wait_send()
        r_copy(g, ra, f, 2, far_id).wait_send()
        r_copy(g, ra, far, 3, near_id).wait_send()

    sent = CHUNK - SHIPPED

    def last_copy(g, size):
        lanes = pl.ds(0, size)
        return pltpu.make_async_remote_copy(
            src_ref=gsend.at[chunks - 1, rows_of(g), lanes], dst_ref=grecv.at[chunks - 1, rows_of(g), lanes],
            send_sem=g_send.at[g, chunks - 1], recv_sem=g_recv.at[g, chunks - 1],
            device_id=partner_id, device_id_type=MESH)

    def for_g_copy(g, k, act):
        @pl.when(k < chunks - 1)
        def _():
            act(g_copy(g, k))

        for which, size in enumerate((sent - EXTRA, sent)):

            @pl.when(jnp.logical_and(k == chunks - 1, core == which))
            def _(size=size):
                act(last_copy(g, size))

    def partner_gradient(g, base, next_load):
        def body(k, slot):
            gsend[k, rows_of(g), :] = jnp.dot(rbt[rows_of(g), :], xbuf[slot], preferred_element_type=jnp.float32)
            for_g_copy(g, k, lambda copy: copy.start())

        steps(base, chunks, other_load, next_load, body)

    def own_columns(g, t, base, next_load):
        lam = lam_col[rows_of(g), 0:1]

        def body(i, slot):
            @pl.when(i == chunks - 1)
            def _():
                r_end(g)
                grecv[chunks - 1, rows_of(g), sent:] = jnp.dot(
                    ra[rows_of(g), :], xbuf[slot, :, EXTRA:EXTRA + SHIPPED], preferred_element_type=jnp.float32)

                @pl.when(core == 0)
                def _():
                    grecv[chunks - 1, rows_of(g), sent - EXTRA:sent] = jnp.dot(
                        ra[rows_of(g), :], xbuf[slot, :, 0:EXTRA], preferred_element_type=jnp.float32)

            @pl.when(i != chunks - 1)
            def _():
                k = i - i // chunks
                for_g_copy(g, k, lambda copy: copy.wait_recv())

                @pl.when(t > 0)
                def _():
                    s_copy(g, k).wait_send()

                mine = jnp.dot(rbt[rows_of(g), :], xbuf[slot], preferred_element_type=jnp.float32)
                weights = wt[k, rows_of(g), :]
                gradient = (mine + grecv[k, rows_of(g), :]) * (1.0 / total_rows)
                lanes = eta_ref.shape[1]
                first = (own * chunks + k) * (CHUNK // lanes)
                eta = jnp.concatenate([eta_ref[pl.ds(first + j, 1), :] for j in range(CHUNK // lanes)], axis=1)
                delta = eta * (gradient - lam * weights)
                wt[k, rows_of(g), :] = weights + STEP_WEIGHT * delta
                delta_b = delta.astype(jnp.bfloat16)
                sbuf[k, rows_of(g), :] = delta_b
                ut[rows_of(g), :] += dot_t(delta_b, xbuf[slot])
                s_copy(g, k).start()

        steps(base, chunks + 1, own_load, next_load, body)

    def partner_columns(g, base, next_load, more=None):
        def body(k, slot):
            s_copy(g, k).wait_recv()
            for_g_copy(g, k, lambda copy: copy.wait_send())
            ut[rows_of(g), :] += dot_t(sbuf[chunks + k, rows_of(g), :], xbuf[slot])

        steps(base, chunks, other_load, next_load, body, more)

    first_forward(last, 0)
    first_end(last - 1, 0)
    first_end(last, 0)
    r_begin(0)
    first_forward(last, 1)
    partner_gradient(0, blocks, other_load)
    first_end(last - 1, 1)
    first_end(last, 1)
    r_begin(1)
    partner_gradient(1, blocks, own_load)

    eta_load.wait()
    for k in range(ahead):
        w0_load(own * chunks + k, k).start()

    def keep(k, carry):
        @pl.when(k + ahead < chunks)
        def _():
            w0_load(own * chunks + k + ahead, (k + ahead) % SLOTS).start()

        w0_load(own * chunks + k, k % SLOTS).wait()
        wt[k] = w0buf[k % SLOTS].T
        return carry

    lax.fori_loop(0, chunks, keep, 0)
    for_ship(lambda where: ship(where).wait())
    r_spread(0)

    def w_store(ref, first, n, k):
        rows = pl.ds(pl.multiple_of(k * CHUNK, CHUNK), CHUNK)
        slot = (first + k) % SLOTS
        return pltpu.make_async_copy(w0buf.at[slot], ref.at[rows, :], out_sem.at[slot])

    def w_copy(k):
        rows = pl.ds(pl.multiple_of(k * CHUNK, CHUNK), CHUNK)
        slot = k % SLOTS
        return pltpu.make_async_remote_copy(
            src_ref=w0buf.at[slot], dst_ref=w_far.at[rows, :], send_sem=w_send.at[slot], recv_sem=w_recv.at[slot],
            device_id=partner_id, device_id_type=MESH)

    def w_send_all():
        for k in range(KEPT):
            w_copy(k).start()

    def w_out():
        first = 0
        for ref, n in (*zip(w_pieces, PIECES), (w_near, KEPT)):

            def put(k, carry, ref=ref, n=n, first=first):
                chunk = first + k
                slot = chunk % SLOTS

                @pl.when(chunk >= SLOTS)
                def _():
                    w_store(ref, first, n, k).wait()

                w0buf[slot] = wt[chunk].T
                w_store(ref, first, n, k).start()
                return carry

            lax.fori_loop(0, n, put, 0)
            first += n

        @pl.when(core == 0)
        def _():
            w_send_all()

    def sweep(t, carry):
        parity = (t + 1) % 2
        more = t < SWEEPS - 1
        at = t * (6 * chunks + 2)
        own_columns(0, t, at, own_load)
        r_spread(1)
        own_columns(1, t, at + chunks + 1, other_load)

        @pl.when(jnp.logical_not(more))
        def _():
            w_out()

        at = at + 2 * chunks + 2
        partner_columns(0, at, other_load)
        u_begin(parity, 0)
        u_end(parity, 0)

        @pl.when(more)
        def _():
            r_begin(0)
            partner_gradient(0, at, other_load)

        partner_columns(1, at, other_load, more)

        @pl.when(more)
        def _():
            r_spread(0)

        u_begin(parity, 1)
        u_end(parity, 1)

        @pl.when(more)
        def _():
            r_begin(1)
            partner_gradient(1, at, own_load)

        return carry

    lax.fori_loop(0, SWEEPS, sweep, 0)
    r_stores = []
    for i in range(2):
        w0buf[SLOTS + i] = rt[:, i * CHUNK:(i + 1) * CHUNK].T
        r_stores.append(
            pltpu.make_async_copy(w0buf.at[SLOTS + i], r_hbm.at[pl.ds(i * CHUNK, CHUNK), :], in_sem.at[i]))
        r_stores[i].start()

    @pl.when(core == 0)
    def _():
        for k in range(KEPT - 1):
            w_copy(k).wait_send()
        pl.semaphore_signal(turn_sem, inc=1, device_id=near_id, device_id_type=MESH)
        w_copy(KEPT - 1).wait_send()

    @pl.when(core == 1)
    def _():
        pl.semaphore_wait(turn_sem, 1)
        w_send_all()
        for k in range(KEPT):
            w_copy(k).wait_send()


    def drain(k, carry):
        for g in range(len(GROUPS)):
            s_copy(g, k).wait_send()
        return carry

    lax.fori_loop(0, chunks, drain, 0)
    for k in range(KEPT):
        w_store(w_near, sum(PIECES), KEPT, k).wait()
        w_copy(k).wait_recv()
    for store in r_stores:
        store.wait()


def place(result, piece, half, first, shape, extra=None):
    rows, width = piece.shape
    halves = shape[0] // CHUNK // 2
    here = pl.BlockSpec((CHUNK, width), lambda i, half_ref: (half_ref[0] * halves + first + i, 0))
    out_shape, out_specs = [jax.ShapeDtypeStruct(shape, piece.dtype)], [here]

    def body(half_ref, piece_ref, other_ref, out_ref, *copied):
        out_ref[...] = piece_ref[...]
        for ref in copied:
            ref[...] = other_ref[...]

    if result is None:
        whole = pl.BlockSpec(extra.shape, lambda i, half_ref: (0, 0))
        out_shape.append(jax.ShapeDtypeStruct(extra.shape, extra.dtype))
        out_specs.append(whole)
        other, other_spec, aliases = extra, whole, {}
    else:
        other, other_spec, aliases = result, pl.BlockSpec(memory_space=pl.ANY), {2: 0}
    return pl.pallas_call(
        body,
        name="place",
        out_shape=out_shape,
        grid_spec=pltpu.PrefetchScalarGridSpec(
            num_scalar_prefetch=1,
            grid=(rows // CHUNK,),
            in_specs=[pl.BlockSpec((CHUNK, width), lambda i, half_ref: (i, 0)), other_spec],
            out_specs=out_specs,
        ),
        input_output_aliases=aliases,
    )(half, piece, other)


def place_last(result, piece, half, first):
    halves = result.shape[0] // CHUNK // 2

    def body(half_ref, piece_ref, result_ref, out_ref, sem):
        start = pl.multiple_of((half_ref[0] * halves + first) * CHUNK, CHUNK)
        copy = pltpu.make_async_copy(piece_ref, out_ref.at[pl.ds(start, piece.shape[0]), :], sem)
        copy.start()
        copy.wait()

    anywhere = pl.BlockSpec(memory_space=pl.ANY)
    return pl.pallas_call(
        body,
        name="place_last",
        out_shape=jax.ShapeDtypeStruct(result.shape, result.dtype),
        grid_spec=pltpu.PrefetchScalarGridSpec(
            num_scalar_prefetch=1, grid=(1,), in_specs=[pl.BlockSpec(memory_space=pltpu.VMEM), anywhere], out_specs=anywhere,
            scratch_shapes=[pltpu.SemaphoreType.DMA]),
        input_output_aliases={2: 0},
    )(half, pltpu.with_memory_space_constraint(piece, pltpu.VMEM), result)


def solution(mesh):
    samp_size = mesh.shape["samp"]
    design_spec = P(("problem", "samp"), "feat")
    rows_spec = P(("problem", "samp"), None)
    coef_spec = P(("problem", "feat"), None)
    step_spec = P(("problem", "feat"))
    ridge_spec = P("problem")

    def local_sweeps(design, targets, coef_init, step_sizes, ridge_weights):
        rows, columns = design.shape
        width = targets.shape[1]
        groups = len(GROUPS)
        chunks = columns // CHUNK // samp_size
        bf16, f32 = jnp.bfloat16, jnp.float32
        vmem, dma = pltpu.VMEM, pltpu.SemaphoreType.DMA
        in_hbm = pl.BlockSpec(memory_space=pltpu.HBM)
        sizes = (KEPT, KEPT, *PIECES)
        resid, _, near, far, *pieces = pl.pallas_call(
            functools.partial(sweep_kernel, rows * samp_size),
            name="sweeps",
            out_shape=(
                jax.ShapeDtypeStruct((rows, width), f32),
                jax.ShapeDtypeStruct((rows, EXTRA + SHIPPED), bf16),
                *(jax.ShapeDtypeStruct((n * CHUNK, width), f32) for n in sizes),
            ),
            in_specs=[in_hbm] * 5,
            out_specs=(in_hbm,) * (2 + len(sizes)),
            scratch_shapes=[
                vmem((SLOTS, rows, CHUNK), bf16),
                vmem((2, CHUNK, rows // ROW_BLOCKS), bf16),
                vmem((SLOTS + 2, CHUNK, width), f32),
                vmem((chunks, width, CHUNK), f32),
                vmem((chunks, width, CHUNK), f32),
                vmem((2 * chunks, width, CHUNK), bf16),
                vmem((chunks, width, CHUNK), f32),
                vmem((width, rows), f32),
                vmem((width, rows // ROW_BLOCKS), f32),
                vmem((width, rows), f32),
                vmem((width, rows), bf16),
                vmem((width, rows), bf16),
                vmem((2, 4, width, rows), bf16),
                vmem((columns // 128, 128), f32),
                vmem((1, width), f32),
                vmem((width, width), f32),
                dma((SLOTS, ROW_BLOCKS)),
                dma((SLOTS + 2,)),
                dma((2,)),
                dma((2,)),
                dma((groups, 4)),
                dma((groups, 4)),
                dma((groups, chunks)),
                dma((groups, chunks)),
                dma((groups, chunks)),
                dma((groups, chunks)),
                dma((ROW_BLOCKS, groups, 3)),
                dma((ROW_BLOCKS, groups, 3)),
                dma((2, groups, 3)),
                dma((2, groups, 3)),
                dma((SLOTS,)),
                dma((SLOTS,)),
                dma((SLOTS,)),
                pltpu.SemaphoreType.REGULAR,
            ],
            compiler_params=pltpu.CompilerParams(
                collective_id=0, has_side_effects=True, vmem_limit_bytes=67_000_000),
        )(design, targets, coef_init, step_sizes.reshape(columns // 128, 128), ridge_weights.reshape(1, width))
        here = lax.axis_index("samp").astype(jnp.int32).reshape(1)
        swap = [(i, samp_size - 1 - i) for i in range(samp_size)]
        arrived = [lax.ppermute(piece, "samp", swap) for piece in pieces]
        shape = (columns, width)
        coef, resid = place(None, near, here, sum(PIECES), shape, resid)
        for half, parts in ((here, pieces), (1 - here, arrived)):
            first = 0
            for piece, n in zip(parts, PIECES):
                if half is not here and first + n == sum(PIECES):
                    coef = place_last(coef, piece, half, first)
                else:
                    (coef,) = place(coef, piece, half, first, shape)
                if half is here and first == 0:
                    (coef,) = place(coef, far, 1 - here, sum(PIECES), shape)
                first += n
        return coef, resid

    return jax.shard_map(
        local_sweeps, mesh=mesh, in_specs=(design_spec, rows_spec, coef_spec, step_spec, ridge_spec),
        out_specs=(coef_spec, rows_spec), check_vma=False)
```

```python
import functools

import jax
import jax.numpy as jnp
from jax import lax
from jax.experimental import pallas as pl
from jax.experimental.pallas import tpu as pltpu
from jax.sharding import PartitionSpec as P

SWEEPS = 4
STEP_WEIGHT = 0.5
CHUNK = 1024
SLOTS = 4
GROUPS = ((0, 48), (48, 80))
SHIPPED = 512
EXTRA = 128
BLOCKS = ((4, 4), (4, 4), (4, 4), (4, 4))
KEPT = 4
PIECES = (6, 5, 1)
MESH = pl.DeviceIdType.MESH


def dot_t(left, right):
    return lax.dot_general(left, right, (((1,), (1,)), ((), ())), preferred_element_type=jnp.float32)


def sweep_kernel(
    total_rows, x_hbm, y_hbm, w0_hbm, eta_hbm, lam_hbm,
    r_hbm, shipped_hbm, w_near, w_far, *rest,
):
    w_pieces, rest = rest[: len(PIECES)], rest[len(PIECES):]
    (
        xbuf, turned, w0buf, gsend, grecv, sbuf, wt, ut, acc, rt, rbt, ra, uall, eta_ref, lam_ref, lam_col,
        x_sem, w0_sem, in_sem, ship_sem, e_send, e_recv, p_send, p_recv, r_send, r_recv, g_send, g_recv, s_send, s_recv, f_send, f_recv, u_send, u_recv, w_send, w_recv, out_sem, turn_sem,
    ) = rest
    z, s, f = lax.axis_index("problem"), lax.axis_index("samp"), lax.axis_index("feat")
    chunks, targets, _ = wt.shape
    core, chip = f % 2, f // 2
    near = chip * 2 + (1 - core)
    far = (1 - chip) * 2 + core
    partner_id = (z, 1 - s, f)
    near_id, far_id = (z, s, near), (z, s, far)
    own, other = s, 1 - s

    barrier = pltpu.get_barrier_semaphore()
    for device in (partner_id, near_id, far_id):
        pl.semaphore_signal(barrier, inc=1, device_id=device, device_id_type=MESH)

    def columns_of(chunk):
        return pl.ds(pl.multiple_of(chunk * CHUNK, CHUNK), CHUNK)

    def x_load(chunk, slot):
        return pltpu.make_async_copy(x_hbm.at[:, columns_of(chunk)], xbuf.at[slot], x_sem.at[slot, 0])

    def w0_load(chunk, slot):
        return pltpu.make_async_copy(w0_hbm.at[columns_of(chunk), :], w0buf.at[slot], w0_sem.at[slot])

    def part(ref, g, k):
        return ref.at[k, pl.ds(*GROUPS[g]), :]

    def rows_of(g):
        return pl.ds(*GROUPS[g])

    def g_copy(g, k):
        return pltpu.make_async_remote_copy(
            src_ref=part(gsend, g, k), dst_ref=part(grecv, g, k), send_sem=g_send.at[g, k], recv_sem=g_recv.at[g, k],
            device_id=partner_id, device_id_type=MESH)

    def s_copy(g, k):
        return pltpu.make_async_remote_copy(
            src_ref=part(sbuf, g, k), dst_ref=part(sbuf, g, chunks + k), send_sem=s_send.at[g, k], recv_sem=s_recv.at[g, k],
            device_id=partner_id, device_id_type=MESH)

    def u_copy(parity, g, slot, which, device):
        rows = uall.at[parity, slot, rows_of(g), :]
        return pltpu.make_async_remote_copy(
            src_ref=rows, dst_ref=rows,
            send_sem=u_send.at[parity, g, which], recv_sem=u_recv.at[parity, g, which],
            device_id=device, device_id_type=MESH)

    ahead = SLOTS - 1

    def start(copy):
        copy.start(priority=1)

    def wait(copy):
        copy.wait()

    def other_load(i, slot, act):
        act(x_load(other * chunks + i, slot))

    def for_ship(act):
        @pl.when(core == 0)
        def _():
            act(pl.ds(0, EXTRA + SHIPPED))

        @pl.when(core == 1)
        def _():
            act(pl.ds(EXTRA, SHIPPED))

    def own_load(i, slot, act):
        @pl.when(i != chunks - 1)
        def _():
            act(x_load(own * chunks + i - i // chunks, slot))

        @pl.when(i == chunks - 1)
        def _():
            for_ship(
                lambda where: act(
                    pltpu.make_async_copy(shipped_hbm.at[:, where], xbuf.at[slot, :, where], x_sem.at[slot, 0])))

    def steps(base, count, load, next_load, body, more=None):
        def step(i, carry):
            upcoming = i + ahead
            slot = (base + upcoming) % SLOTS

            @pl.when(upcoming < count)
            def _():
                load(upcoming, slot, start)

            wanted = upcoming >= count
            if more is not None:
                wanted = jnp.logical_and(wanted, more)

            @pl.when(wanted)
            def _():
                next_load(upcoming - count, slot, start)

            load(i, (base + i) % SLOTS, wait)
            body(i, (base + i) % SLOTS)
            return carry

        lax.fori_loop(0, count, step, 0)

    sizes = [x_hbm.shape[0] // share for share, _ in BLOCKS]
    firsts = [sum(sizes[:i]) for i in range(len(sizes))]
    widths = [width for _, width in BLOCKS]
    counts = [2 * chunks // width for width in widths]
    bases = [sum(counts[:i]) for i in range(len(counts))]
    blocks = sum(counts)
    rows, width, passes = sizes[0], widths[0], counts[0]
    pairs = w0buf.shape[0] // 2

    def tile_load(block, step, q):
        slot, size, i = step % SLOTS, sizes[block], step - bases[block]
        return pltpu.make_async_copy(
            x_hbm.at[pl.ds(firsts[block], size), columns_of(i * widths[block] + q)],
            xbuf.at[slot, pl.ds(q * size, size), :], x_sem.at[slot, q])

    def tiles_ahead(block, step):
        upcoming = step + ahead
        reach = bases[block] + counts[block] + ahead
        for later in range(block, len(BLOCKS)):
            if bases[later] < reach:

                @pl.when(jnp.logical_and(upcoming >= bases[later], upcoming < bases[later] + counts[later]))
                def _(later=later):
                    for q in range(widths[later]):
                        tile_load(later, upcoming, q).start(priority=1)

        if blocks < reach:

            @pl.when(upcoming >= blocks)
            def _():
                x_load(other * chunks + upcoming - blocks, upcoming % SLOTS).start(priority=1)

    def w0_pair(pair, q):
        return w0_load(2 * pair + q, 2 * (pair % pairs) + q)

    eta_load = pltpu.make_async_copy(eta_hbm, eta_ref, in_sem.at[0])
    lam_load = pltpu.make_async_copy(lam_hbm, lam_ref, in_sem.at[1])
    halves = [
        pltpu.make_async_copy(
            y_hbm.at[pl.ds(i * CHUNK, CHUNK), :], w0buf.at[2 * pairs - 2 + i], w0_sem.at[2 * pairs - 2 + i])
        for i in range(2)
    ]
    end_shipped = (other + 1) * chunks * CHUNK

    def ship(where):
        first = end_shipped - EXTRA - SHIPPED + where.start
        return pltpu.make_async_remote_copy(
            src_ref=x_hbm.at[:, pl.ds(pl.multiple_of(first, 128), where.size)], dst_ref=shipped_hbm.at[:, where],
            send_sem=ship_sem.at[0], recv_sem=ship_sem.at[1], device_id=partner_id, device_id_type=MESH)

    for load in (*halves, lam_load, eta_load):
        load.start()
    for pair in range(pairs - 1):
        for q in range(2):
            w0_pair(pair, q).start()
    for step in range(ahead):
        for q in range(width):
            tile_load(0, step, q).start(priority=1)
    pl.semaphore_wait(barrier, 3)

    for_ship(lambda where: ship(where).start())
    ut[...] = jnp.zeros_like(ut)
    acc[...] = jnp.zeros_like(acc)
    for i, load in enumerate(halves):
        load.wait()
        rt[:, i * CHUNK:(i + 1) * CHUNK] = w0buf[2 * pairs - 2 + i].T
    lam_load.wait()
    lam_col[...] = jnp.broadcast_to(lam_ref[0:1, :], (targets, targets)).T

    def first_pass(pair, carry):
        @pl.when(pair % (width // 2) == 0)
        def _():
            tiles_ahead(0, pair // (width // 2))

        @pl.when(pair + pairs - 1 < chunks)
        def _():
            for q in range(2):
                w0_pair(pair + pairs - 1, q).start()

        slot = pair // (width // 2) % SLOTS
        first = pair % (width // 2) * 2
        total = acc[...]
        for q in range(2):
            w0_pair(pair, q).wait()
            tile_load(0, pair // (width // 2), first + q).wait()
        for q in range(2):
            weights = w0buf[2 * (pair % pairs) + q].T.astype(jnp.bfloat16)
            sbuf[2 * pair + q] = weights
            where = pl.ds(pl.multiple_of((first + q) * rows, rows), rows)
            total += dot_t(weights, xbuf[slot, where, :])
        acc[...] = total
        return carry

    def block_product(weights, tiles):
        plain = len(tiles) // 2
        size = tiles[0].shape[0]
        per_slab = turned.shape[2] // size
        slabs = [turned.at[q // per_slab, :, pl.ds(q % per_slab * size, size)] for q in range(len(tiles) - plain)]
        for slab, tile in zip(slabs, tiles[plain:]):
            slab[...] = tile.T
        total = sum(dot_t(weight, tile) for weight, tile in zip(weights[:plain], tiles))
        for slab, weight in zip(slabs, weights[plain:]):
            total += jnp.dot(weight, slab[...], preferred_element_type=jnp.float32)
        return total

    def later_pass(block):
        size, some = sizes[block], range(widths[block])

        def step_(i, inner):
            step = bases[block] + i
            tiles_ahead(block, step)
            for q in some:
                tile_load(block, step, q).wait()
            slot = step % SLOTS
            acc[:, 0:size] += block_product(
                [sbuf[i * widths[block] + q] for q in some], [xbuf[slot, q * size:(q + 1) * size, :] for q in some])
            return inner

        lax.fori_loop(0, counts[block], step_, 0)

    def lanes_of(block):
        return pl.ds(firsts[block], sizes[block])

    def first_copy(block, g, slot, which, device):
        ref = uall.at[0, slot, rows_of(g), lanes_of(block)]
        return pltpu.make_async_remote_copy(
            src_ref=ref, dst_ref=ref, send_sem=f_send.at[block, g, which], recv_sem=f_recv.at[block, g, which],
            device_id=device, device_id_type=MESH)

    def first_begin(block):
        uall[0, f, :, lanes_of(block)] = acc[:, 0:sizes[block]].astype(jnp.bfloat16)
        acc[...] = jnp.zeros_like(acc)
        for g in range(len(GROUPS)):
            first_copy(block, g, f, 0, near_id).start()
            first_copy(block, g, f, 1, far_id).start()

    def first_forward(block, g):
        first_copy(block, g, far, 1, far_id).wait_recv()
        first_copy(block, g, far, 2, near_id).start()

    def first_end(block, g):
        first_copy(block, g, near, 0, near_id).wait_recv()
        first_copy(block, g, far, 2, near_id).wait_recv()
        total = uall[0, 0, rows_of(g), lanes_of(block)].astype(jnp.float32)
        for j in range(1, 4):
            total += uall[0, j, rows_of(g), lanes_of(block)].astype(jnp.float32)
        new = rt[rows_of(g), lanes_of(block)] - total
        rt[rows_of(g), lanes_of(block)] = new
        rbt[rows_of(g), lanes_of(block)] = new.astype(jnp.bfloat16)
        first_copy(block, g, f, 0, near_id).wait_send()
        first_copy(block, g, f, 1, far_id).wait_send()
        first_copy(block, g, far, 2, near_id).wait_send()

    piece = rows // 4

    def first_r(block, g=None):
        rows_g = rows_of(g) if g is not None else pl.ds(0, targets)
        which = block + (g or 0)
        lanes = pl.ds(pl.multiple_of(block * rows + f * piece, piece), piece)
        return pltpu.make_async_remote_copy(
            src_ref=rbt.at[rows_g, lanes], dst_ref=ra.at[rows_g, lanes],
            send_sem=e_send.at[which], recv_sem=e_recv.at[which], device_id=partner_id, device_id_type=MESH)

    lax.fori_loop(0, chunks, first_pass, 0)
    last = len(BLOCKS) - 1
    for block in range(len(BLOCKS)):
        if block:
            later_pass(block)
        first_begin(block)
        for g in range(len(GROUPS)):
            if block >= 1:
                first_forward(block - 1, g)
            if block >= 2:
                first_end(block - 2, g)
        if 2 <= block < 4:
            first_r(block - 2).start()

    def u_begin(parity, g):
        uall[parity, f, rows_of(g), :] = ut[rows_of(g), :].astype(jnp.bfloat16)
        ut[rows_of(g), :] = jnp.zeros((GROUPS[g][1], ut.shape[1]), jnp.float32)
        u_copy(parity, g, f, 0, near_id).start()
        u_copy(parity, g, f, 1, far_id).start()

    def u_end(parity, g):
        u_copy(parity, g, far, 1, far_id).wait_recv()
        u_copy(parity, g, far, 2, near_id).start()
        u_copy(parity, g, near, 0, near_id).wait_recv()
        u_copy(parity, g, far, 2, near_id).wait_recv()
        total = uall[parity, 0, rows_of(g), :].astype(jnp.float32)
        for block in range(1, 4):
            total += uall[parity, block, rows_of(g), :].astype(jnp.float32)
        new = rt[rows_of(g), :] - STEP_WEIGHT * total
        rt[rows_of(g), :] = new
        rbt[rows_of(g), :] = new.astype(jnp.bfloat16)
        u_copy(parity, g, f, 0, near_id).wait_send()
        u_copy(parity, g, f, 1, far_id).wait_send()
        u_copy(parity, g, far, 2, near_id).wait_send()

    quarter = ra.shape[1] // 4

    def r_copy(g, source, of, which, device):
        lanes = pl.ds(pl.multiple_of(of * quarter, quarter), quarter)
        return pltpu.make_async_remote_copy(
            src_ref=source.at[rows_of(g), lanes], dst_ref=ra.at[rows_of(g), lanes],
            send_sem=r_send.at[g, which], recv_sem=r_recv.at[g, which], device_id=device, device_id_type=MESH)

    def r_begin(g):
        r_copy(g, rbt, f, 0, partner_id).start()

    def r_spread(g):
        r_copy(g, rbt, f, 0, partner_id).wait()
        r_copy(g, ra, f, 1, near_id).start()
        r_copy(g, ra, f, 2, far_id).start()

    def r_end(g):
        r_copy(g, ra, far, 2, far_id).wait_recv()
        r_copy(g, ra, far, 3, near_id).start()
        r_copy(g, ra, near, 1, near_id).wait_recv()
        r_copy(g, ra, far, 3, near_id).wait_recv()
        r_copy(g, ra, f, 1, near_id).wait_send()
        r_copy(g, ra, f, 2, far_id).wait_send()
        r_copy(g, ra, far, 3, near_id).wait_send()

    sent = CHUNK - SHIPPED

    def last_copy(g, size):
        lanes = pl.ds(0, size)
        return pltpu.make_async_remote_copy(
            src_ref=gsend.at[chunks - 1, rows_of(g), lanes], dst_ref=grecv.at[chunks - 1, rows_of(g), lanes],
            send_sem=g_send.at[g, chunks - 1], recv_sem=g_recv.at[g, chunks - 1],
            device_id=partner_id, device_id_type=MESH)

    def for_g_copy(g, k, act):
        @pl.when(k < chunks - 1)
        def _():
            act(g_copy(g, k))

        for which, size in enumerate((sent - EXTRA, sent)):

            @pl.when(jnp.logical_and(k == chunks - 1, core == which))
            def _(size=size):
                act(last_copy(g, size))

    def partner_gradient(g, base, next_load):
        def body(k, slot):
            gsend[k, rows_of(g), :] = jnp.dot(rbt[rows_of(g), :], xbuf[slot], preferred_element_type=jnp.float32)
            for_g_copy(g, k, lambda copy: copy.start())

        steps(base, chunks, other_load, next_load, body)

    def own_columns(g, t, base, next_load):
        lam = lam_col[rows_of(g), 0:1]

        def body(i, slot):
            @pl.when(i == chunks - 1)
            def _():
                @pl.when(t > 0)
                def _():
                    r_end(g)

                grecv[chunks - 1, rows_of(g), sent:] = jnp.dot(
                    ra[rows_of(g), :], xbuf[slot, :, EXTRA:EXTRA + SHIPPED], preferred_element_type=jnp.float32)

                @pl.when(core == 0)
                def _():
                    grecv[chunks - 1, rows_of(g), sent - EXTRA:sent] = jnp.dot(
                        ra[rows_of(g), :], xbuf[slot, :, 0:EXTRA], preferred_element_type=jnp.float32)

            @pl.when(i != chunks - 1)
            def _():
                k = i - i // chunks
                for_g_copy(g, k, lambda copy: copy.wait_recv())

                @pl.when(t > 0)
                def _():
                    s_copy(g, k).wait_send()

                mine = jnp.dot(rbt[rows_of(g), :], xbuf[slot], preferred_element_type=jnp.float32)
                weights = wt[k, rows_of(g), :]
                gradient = (mine + grecv[k, rows_of(g), :]) * (1.0 / total_rows)
                lanes = eta_ref.shape[1]
                first = (own * chunks + k) * (CHUNK // lanes)
                eta = jnp.concatenate([eta_ref[pl.ds(first + j, 1), :] for j in range(CHUNK // lanes)], axis=1)
                delta = eta * (gradient - lam * weights)
                wt[k, rows_of(g), :] = weights + STEP_WEIGHT * delta
                delta_b = delta.astype(jnp.bfloat16)
                sbuf[k, rows_of(g), :] = delta_b
                ut[rows_of(g), :] += dot_t(delta_b, xbuf[slot])
                s_copy(g, k).start()

        steps(base, chunks + 1, own_load, next_load, body)

    def partner_columns(g, base, next_load, more=None):
        def body(k, slot):
            s_copy(g, k).wait_recv()
            for_g_copy(g, k, lambda copy: copy.wait_send())
            ut[rows_of(g), :] += dot_t(sbuf[chunks + k, rows_of(g), :], xbuf[slot])

        steps(base, chunks, other_load, next_load, body, more)

    first_forward(last, 0)
    for g in range(len(GROUPS)):
        first_end(last - 1, g)
    first_r(2).start()
    first_end(last, 0)
    first_r(3, 0).start()
    first_forward(last, 1)
    partner_gradient(0, blocks, other_load)
    first_end(last, 1)
    first_r(3, 1).start()
    partner_gradient(1, blocks + chunks, own_load)

    def first_r_pass(block, of, which, device):
        lanes = pl.ds(pl.multiple_of(block * rows + of * piece, piece), piece)
        return pltpu.make_async_remote_copy(
            src_ref=ra.at[:, lanes], dst_ref=ra.at[:, lanes],
            send_sem=p_send.at[block, which], recv_sem=p_recv.at[block, which], device_id=device, device_id_type=MESH)

    def first_r_spread():
        for block in range(3):
            first_r(block).wait()
        for g in range(len(GROUPS)):
            first_r(3, g).wait()
        for block in range(4):
            first_r_pass(block, f, 0, near_id).start()
            first_r_pass(block, f, 1, far_id).start()
        for block in range(4):
            first_r_pass(block, far, 1, far_id).wait_recv()
        for block in range(4):
            first_r_pass(block, far, 2, near_id).start()
        for block in range(4):
            first_r_pass(block, near, 0, near_id).wait_recv()
            first_r_pass(block, far, 2, near_id).wait_recv()
            first_r_pass(block, f, 0, near_id).wait_send()
            first_r_pass(block, f, 1, far_id).wait_send()
            first_r_pass(block, far, 2, near_id).wait_send()

    eta_load.wait()
    for k in range(ahead):
        w0_load(own * chunks + k, k).start()

    def keep(k, carry):
        @pl.when(k + ahead < chunks)
        def _():
            w0_load(own * chunks + k + ahead, (k + ahead) % SLOTS).start()

        w0_load(own * chunks + k, k % SLOTS).wait()
        wt[k] = w0buf[k % SLOTS].T
        return carry

    lax.fori_loop(0, chunks, keep, 0)
    for_ship(lambda where: ship(where).wait())
    first_r_spread()

    def w_store(ref, first, n, k):
        rows = pl.ds(pl.multiple_of(k * CHUNK, CHUNK), CHUNK)
        slot = (first + k) % SLOTS
        return pltpu.make_async_copy(w0buf.at[slot], ref.at[rows, :], out_sem.at[slot])

    def w_copy(k):
        rows = pl.ds(pl.multiple_of(k * CHUNK, CHUNK), CHUNK)
        slot = k % SLOTS
        return pltpu.make_async_remote_copy(
            src_ref=w0buf.at[slot], dst_ref=w_far.at[rows, :], send_sem=w_send.at[slot], recv_sem=w_recv.at[slot],
            device_id=partner_id, device_id_type=MESH)

    def w_send_all():
        for k in range(KEPT):
            w_copy(k).start()

    def w_out():
        first = 0
        for ref, n in (*zip(w_pieces, PIECES), (w_near, KEPT)):

            def put(k, carry, ref=ref, n=n, first=first):
                chunk = first + k
                slot = chunk % SLOTS

                @pl.when(chunk >= SLOTS)
                def _():
                    w_store(ref, first, n, k).wait()

                w0buf[slot] = wt[chunk].T
                w_store(ref, first, n, k).start()
                return carry

            lax.fori_loop(0, n, put, 0)
            first += n

        @pl.when(core == 0)
        def _():
            w_send_all()

    def sweep(t, carry):
        parity = (t + 1) % 2
        more = t < SWEEPS - 1
        at = blocks + 2 * chunks + t * (6 * chunks + 2)
        own_columns(0, t, at, own_load)

        @pl.when(t > 0)
        def _():
            r_spread(1)

        own_columns(1, t, at + chunks + 1, other_load)

        @pl.when(jnp.logical_not(more))
        def _():
            w_out()

        at = at + 2 * chunks + 2
        partner_columns(0, at, other_load)
        u_begin(parity, 0)
        u_end(parity, 0)

        @pl.when(more)
        def _():
            r_begin(0)
            partner_gradient(0, at, other_load)

        partner_columns(1, at, other_load, more)

        @pl.when(more)
        def _():
            r_spread(0)

        u_begin(parity, 1)
        u_end(parity, 1)

        @pl.when(more)
        def _():
            r_begin(1)
            partner_gradient(1, at, own_load)

        return carry

    lax.fori_loop(0, SWEEPS, sweep, 0)
    r_stores = []
    for i in range(2):
        w0buf[SLOTS + i] = rt[:, i * CHUNK:(i + 1) * CHUNK].T
        r_stores.append(
            pltpu.make_async_copy(w0buf.at[SLOTS + i], r_hbm.at[pl.ds(i * CHUNK, CHUNK), :], in_sem.at[i]))
        r_stores[i].start()

    @pl.when(core == 0)
    def _():
        for k in range(KEPT - 1):
            w_copy(k).wait_send()
        pl.semaphore_signal(turn_sem, inc=1, device_id=near_id, device_id_type=MESH)
        w_copy(KEPT - 1).wait_send()

    @pl.when(core == 1)
    def _():
        pl.semaphore_wait(turn_sem, 1)
        w_send_all()
        for k in range(KEPT):
            w_copy(k).wait_send()


    def drain(k, carry):
        for g in range(len(GROUPS)):
            s_copy(g, k).wait_send()
        return carry

    lax.fori_loop(0, chunks, drain, 0)
    for k in range(KEPT):
        w_store(w_near, sum(PIECES), KEPT, k).wait()
        w_copy(k).wait_recv()
    for store in r_stores:
        store.wait()


def place(result, piece, half, first, shape, extra=None):
    rows, width = piece.shape
    halves = shape[0] // CHUNK // 2
    here = pl.BlockSpec((CHUNK, width), lambda i, half_ref: (half_ref[0] * halves + first + i, 0))
    out_shape, out_specs = [jax.ShapeDtypeStruct(shape, piece.dtype)], [here]

    def body(half_ref, piece_ref, other_ref, out_ref, *copied):
        out_ref[...] = piece_ref[...]
        for ref in copied:
            ref[...] = other_ref[...]

    if result is None:
        whole = pl.BlockSpec(extra.shape, lambda i, half_ref: (0, 0))
        out_shape.append(jax.ShapeDtypeStruct(extra.shape, extra.dtype))
        out_specs.append(whole)
        other, other_spec, aliases = extra, whole, {}
    else:
        other, other_spec, aliases = result, pl.BlockSpec(memory_space=pl.ANY), {2: 0}
    return pl.pallas_call(
        body,
        name="place",
        out_shape=out_shape,
        grid_spec=pltpu.PrefetchScalarGridSpec(
            num_scalar_prefetch=1,
            grid=(rows // CHUNK,),
            in_specs=[pl.BlockSpec((CHUNK, width), lambda i, half_ref: (i, 0)), other_spec],
            out_specs=out_specs,
        ),
        input_output_aliases=aliases,
    )(half, piece, other)


def place_last(result, piece, half, first):
    halves = result.shape[0] // CHUNK // 2

    def body(half_ref, piece_ref, result_ref, out_ref, sem):
        start = pl.multiple_of((half_ref[0] * halves + first) * CHUNK, CHUNK)
        copy = pltpu.make_async_copy(piece_ref, out_ref.at[pl.ds(start, piece.shape[0]), :], sem)
        copy.start()
        copy.wait()

    anywhere = pl.BlockSpec(memory_space=pl.ANY)
    return pl.pallas_call(
        body,
        name="place_last",
        out_shape=jax.ShapeDtypeStruct(result.shape, result.dtype),
        grid_spec=pltpu.PrefetchScalarGridSpec(
            num_scalar_prefetch=1, grid=(1,), in_specs=[pl.BlockSpec(memory_space=pltpu.VMEM), anywhere], out_specs=anywhere,
            scratch_shapes=[pltpu.SemaphoreType.DMA]),
        input_output_aliases={2: 0},
    )(half, pltpu.with_memory_space_constraint(piece, pltpu.VMEM), result)


def solution(mesh):
    samp_size = mesh.shape["samp"]
    design_spec = P(("problem", "samp"), "feat")
    rows_spec = P(("problem", "samp"), None)
    coef_spec = P(("problem", "feat"), None)
    step_spec = P(("problem", "feat"))
    ridge_spec = P("problem")

    def local_sweeps(design, targets, coef_init, step_sizes, ridge_weights):
        rows, columns = design.shape
        width = targets.shape[1]
        groups = len(GROUPS)
        chunks = columns // CHUNK // samp_size
        bf16, f32 = jnp.bfloat16, jnp.float32
        vmem, dma = pltpu.VMEM, pltpu.SemaphoreType.DMA
        in_hbm = pl.BlockSpec(memory_space=pltpu.HBM)
        sizes = (KEPT, KEPT, *PIECES)
        resid, _, near, far, *pieces = pl.pallas_call(
            functools.partial(sweep_kernel, rows * samp_size),
            name="sweeps",
            out_shape=(
                jax.ShapeDtypeStruct((rows, width), f32),
                jax.ShapeDtypeStruct((rows, EXTRA + SHIPPED), bf16),
                *(jax.ShapeDtypeStruct((n * CHUNK, width), f32) for n in sizes),
            ),
            in_specs=[in_hbm] * 5,
            out_specs=(in_hbm,) * (2 + len(sizes)),
            scratch_shapes=[
                vmem((SLOTS, rows, CHUNK), bf16),
                vmem((2, CHUNK, rows // 4), bf16),
                vmem((SLOTS + 2, CHUNK, width), f32),
                vmem((chunks, width, CHUNK), f32),
                vmem((chunks, width, CHUNK), f32),
                vmem((2 * chunks, width, CHUNK), bf16),
                vmem((chunks, width, CHUNK), f32),
                vmem((width, rows), f32),
                vmem((width, rows // 4), f32),
                vmem((width, rows), f32),
                vmem((width, rows), bf16),
                vmem((width, rows), bf16),
                vmem((2, 4, width, rows), bf16),
                vmem((columns // 128, 128), f32),
                vmem((1, width), f32),
                vmem((width, width), f32),
                dma((SLOTS, max(count for _, count in BLOCKS))),
                dma((SLOTS + 2,)),
                dma((2,)),
                dma((2,)),
                dma((4 + groups - 1,)),
                dma((4 + groups - 1,)),
                dma((4, 3)),
                dma((4, 3)),
                dma((groups, 4)),
                dma((groups, 4)),
                dma((groups, chunks)),
                dma((groups, chunks)),
                dma((groups, chunks)),
                dma((groups, chunks)),
                dma((len(BLOCKS), groups, 3)),
                dma((len(BLOCKS), groups, 3)),
                dma((2, groups, 3)),
                dma((2, groups, 3)),
                dma((SLOTS,)),
                dma((SLOTS,)),
                dma((SLOTS,)),
                pltpu.SemaphoreType.REGULAR,
            ],
            compiler_params=pltpu.CompilerParams(
                collective_id=0, has_side_effects=True, vmem_limit_bytes=67_000_000),
        )(design, targets, coef_init, step_sizes.reshape(columns // 128, 128), ridge_weights.reshape(1, width))
        here = lax.axis_index("samp").astype(jnp.int32).reshape(1)
        swap = [(i, samp_size - 1 - i) for i in range(samp_size)]
        arrived = [lax.ppermute(piece, "samp", swap) for piece in pieces]
        shape = (columns, width)
        coef, resid = place(None, near, here, sum(PIECES), shape, resid)
        for half, parts in ((here, pieces), (1 - here, arrived)):
            first = 0
            for piece, n in zip(parts, PIECES):
                if half is not here and first + n == sum(PIECES):
                    coef = place_last(coef, piece, half, first)
                else:
                    (coef,) = place(coef, piece, half, first, shape)
                if half is here and first == 0:
                    (coef,) = place(coef, far, 1 - here, sum(PIECES), shape)
                first += n
        return coef, resid

    return jax.shard_map(
        local_sweeps, mesh=mesh, in_specs=(design_spec, rows_spec, coef_spec, step_spec, ridge_spec),
        out_specs=(coef_spec, rows_spec), check_vma=False)
```
